8 devices in a mesh: rep: 1 (over z), dp: 8 (over x, y, core).
Axes of the slice: x: 2, y: 2, z: 1, core: 2. Of those that a mesh axis runs over, the one named last changes fastest.
Arguments:
- g_w_gate: bfloat16 [8, 2, 1024, 3200], P(('rep', 'dp'))
- g_w_up: bfloat16 [8, 2, 1024, 3200], P(('rep', 'dp'))
- g_w_down: bfloat16 [8, 2, 3200, 1024], P(('rep', 'dp'))
- w_gate: bfloat16 [2, 1024, 3200], replicated
- w_up: bfloat16 [2, 1024, 3200], replicated
- w_down: bfloat16 [2, 3200, 1024], replicated
- m_w_gate: float32 [2, 1024, 3200], P(None, 'dp')
- m_w_up: float32 [2, 1024, 3200], P(None, 'dp')
- m_w_down: float32 [2, 3200, 1024], P(None, 'dp')
- v_w_gate: float32 [2, 1024, 3200], P(None, 'dp')
- v_w_up: float32 [2, 1024, 3200], P(None, 'dp')
- v_w_down: float32 [2, 3200, 1024], P(None, 'dp')
Outputs:
- output 1: bfloat16 [2, 1024, 3200], P('rep')
- output 2: bfloat16 [2, 1024, 3200], P('rep')
- output 3: bfloat16 [2, 3200, 1024], P('rep')
- output 4: float32 [2, 1024, 3200], P('rep', 'dp')
- output 5: float32 [2, 1024, 3200], P('rep', 'dp')
- output 6: float32 [2, 3200, 1024], P('rep', 'dp')
- output 7: float32 [2, 1024, 3200], P('rep', 'dp')
- output 8: float32 [2, 1024, 3200], P('rep', 'dp')
- output 9: float32 [2, 3200, 1024], P('rep', 'dp')
All inputs are finite; a program needn't handle non-finite values.
Results may differ from the reference program's by a relative error of at most 0.022.
Values are sent between devices in bfloat16 or wider.
A program may use at most 2 GiB of HBM per device.

```python
import jax
import jax.numpy as jnp
from jax import lax

DEVICES = 8
D = 1024
FF = 3200
LAYERS = 2
NAMES = ("w_gate", "w_up", "w_down")
SHAPES = {"w_gate": (LAYERS, D, FF), "w_up": (LAYERS, D, FF), "w_down": (LAYERS, FF, D)}


def setup_inputs(seed: int = 0, part: int = 0) -> dict:
    kz, *keys = jax.random.split(jax.random.key(seed), 1 + 5 * len(NAMES))
    loud = 2.0 ** jax.random.uniform(kz, (), jnp.float32, -1.0, 1.0)
    drawn = {}
    for name, key, both in zip(NAMES, keys[:3], keys[3:6], strict=True):
        own = jax.random.normal(jax.random.fold_in(key, part), (DEVICES, *SHAPES[name]), jnp.float32)
        shared = jax.random.normal(jax.random.fold_in(both, part), SHAPES[name], jnp.float32)
        drawn["g_" + name] = (loud * (0.7 * shared / DEVICES + 0.7 * own * DEVICES**-0.5)).astype(jnp.bfloat16)
    for name, key in zip(NAMES, keys[6:9], strict=True):
        drawn[name] = (jax.random.normal(key, SHAPES[name], jnp.float32) * SHAPES[name][1] ** -0.5).astype(jnp.bfloat16)
    for name, key in zip(NAMES, keys[9:12], strict=True):
        drawn["m_" + name] = loud * 0.5 * jax.random.normal(key, SHAPES[name], jnp.float32)
    for name, key in zip(NAMES, keys[12:15], strict=True):
        drawn["v_" + name] = loud * loud * jax.random.uniform(key, SHAPES[name], jnp.float32, 0.5, 1.5)
    return drawn


def adamw(w, m, v, g):
    m = 0.9 * m + 0.1 * g
    v = 0.95 * v + 0.05 * g * g
    step = m * lax.rsqrt(v + 1e-8) + 0.1 * w
    return (w - 0.02 * step).astype(jnp.bfloat16), m, v


def clipped(gradients, sum_of_squares, count):
    factor = jnp.minimum(1.0, 0.5 * lax.rsqrt(sum_of_squares / count + 1e-30))
    return [g * factor for g in gradients]


def reference(g_w_gate, g_w_up, g_w_down, w_gate, w_up, w_down, m_w_gate, m_w_up, m_w_down, v_w_gate, v_w_up, v_w_down):
    def total(terms):
        return lax.scan(lambda so_far, term: (so_far + term.astype(jnp.float32), None), jnp.zeros(terms.shape[1:], jnp.float32), terms)[0]

    gradients = [total(terms).astype(jnp.bfloat16).astype(jnp.float32) for terms in (g_w_gate, g_w_up, g_w_down)]
    gradients = clipped(gradients, sum(jnp.sum(g * g) for g in gradients), sum(g.size for g in gradients))
    new = [
        adamw(w.astype(jnp.float32), m, v, g)
        for w, m, v, g in zip((w_gate, w_up, w_down), (m_w_gate, m_w_up, m_w_down), (v_w_gate, v_w_up, v_w_down), gradients, strict=True)
    ]
    return tuple(one[which] for which in range(3) for one in new)
```

```python
import functools

import jax
import jax.numpy as jnp
from jax import lax
from jax.experimental import pallas as pl
from jax.experimental.pallas import tpu as pltpu
from jax.sharding import PartitionSpec as P

D, FF, LAYERS, N = 1024, 3200, 2, 8
COUNT = 3 * LAYERS * D * FF
BLOCKS = ((0, 0), (0, 1), (1, 0), (1, 1), (2, 0), (2, 1))
AHEAD = 8
WINDOW = 2


def rows_of(b):
    return 128 if b < 4 else 400


def half(b, h):
    rows = rows_of(b)
    split = 64 if b < 4 else (208 if b == 4 else 192)
    return (0, split) if h == 0 else (split, rows - split)


def columns(b):
    return [(i * 640, 640) for i in range(5)] if b < 4 else [(i * 512, 512) for i in range(2)]


def f32(x):
    return x.astype(jnp.float32)


def kernel(gg, gu, gd, wg, wu, wd, mg, mu, md, vg, vu, vd,
           og, ou, od, qg, qu, qd, fac,
           own_a, own_b, part_a, part_b, rec_a, rec_b, mv_a, mv_b, ws_a, ws_b, sq, nrm,
           load_sem, d2d_send, d2d_recv, link_send, link_recv, nrm_send, nrm_recv,
           gat_send, gat_recv, gd_send, gd_recv, wmv_sem, out_sem, g_sem):
    grads, weights, ms, vs, outs, qs = (gg, gu, gd), (wg, wu, wd), (mg, mu, md), (vg, vu, vd), (og, ou, od), (qg, qu, qd)
    me = lax.axis_index("dp")
    x, y, c = lax.div(me, 4), lax.rem(lax.div(me, 2), 2), lax.rem(me, 2)

    def device(r, other=0):
        cx, cy = lax.rem(x + r // 2, 2), lax.rem(y + r % 2, 2)
        return cx * 4 + cy * 2 + (1 - c if other else c)

    def to(index):
        return dict(device_id={"dp": index}, device_id_type=pl.DeviceIdType.MESH)

    across = (device(2), device(1))
    partner = device(0, 1)

    def own(b, r, h, n=None):
        lo, num = half(b, h)
        return (own_a.at[b, r, pl.ds(lo, num)] if b < 4 else own_b.at[b - 4, r, pl.ds(lo, num)])

    def part(b, r, h):
        lo, num = half(b, h)
        return (part_a.at[b, r, pl.ds(lo, num)] if b < 4 else part_b.at[b - 4, r, pl.ds(lo, num)])

    def rec(b, h, k):
        lo, num = half(b, h)
        return (rec_a.at[b, h, k] if b < 4 else rec_b.at[b - 4, h, k, pl.ds(0, num)])

    def span(ref, b, h, dev, lead=()):
        lo, num = half(b, h)
        w, layer = BLOCKS[b]
        return ref[w].at[(*lead, layer, pl.ds(pl.multiple_of(dev * rows_of(b) + lo, 16), num))]

    def mine(ref, b, h):
        lo, num = half(b, h)
        return ref[BLOCKS[b][0]].at[BLOCKS[b][1], pl.ds(lo, num)]

    barrier = pltpu.get_barrier_semaphore()
    for k in range(1, N):
        pl.semaphore_signal(barrier, inc=1, **to(lax.rem(me + k, N)))

    def chip(kind, h):
        return {"S1": 3, "S2": (2, 1)[h], "R": (1, 2)[h], "G": 0}[kind]

    order = [(kind, b, h) for kind in ("S1", "S2", "R", "G") for b in range(6) for h in range(2)]
    place = {step: i for i, step in enumerate(order)}
    loads, d2ds = {}, {}

    def fetch_own(i):
        kind, b, h = order[i]
        r = chip(kind, h)
        loads[i] = pltpu.make_async_copy(span(grads, b, h, device(r), (0,)), own(b, r, h), load_sem.at[i])
        loads[i].start()

    def fetch_part(i):
        kind, b, h = order[i]
        r = chip(kind, h)
        d2ds[i] = pltpu.make_async_remote_copy(
            span(grads, b, h, device(r, 1), (0,)), part(b, r, h), d2d_send.at[i], d2d_recv.at[i], **to(partner))
        d2ds[i].start()

    for i in range(AHEAD):
        fetch_own(i)
    pl.semaphore_wait(barrier, N - 1)
    for i in range(AHEAD):
        fetch_part(i)

    def ready(step):
        i = place[step]
        if i + AHEAD < len(order):
            fetch_own(i + AHEAD)
            fetch_part(i + AHEAD)
        loads[i].wait()
        d2ds[i].wait_recv()

    def add(b, h, r, terms, squares=False):
        num = half(b, h)[1]
        target = own(b, r, h)

        def body(i, carry):
            at = pl.ds(pl.multiple_of(i * 16, 16), 16)
            for lo, width in columns(b):
                total = f32(target[at, pl.ds(lo, width)])
                for t in terms:
                    total = total + f32(t[at, pl.ds(lo, width)])
                rounded = total.astype(jnp.bfloat16)
                target[at, pl.ds(lo, width)] = rounded
                if squares:
                    g = f32(rounded)
                    g = g * g
                    s = g[:, 0:128]
                    for k in range(1, width // 128):
                        s = s + g[:, k * 128:(k + 1) * 128]
                    carry = carry + s
            return carry

        done = lax.fori_loop(0, num // 16, body, jnp.zeros((16, 128), jnp.float32) if squares else 0)
        if squares:
            sq[...] += done

    links = [{}, {}]

    def send(d, i, src, dst):
        if i >= WINDOW:
            links[d][i - WINDOW].wait_send()
        links[d][i] = pltpu.make_async_remote_copy(src, dst, link_send.at[d, i], link_recv.at[d, i], **to(across[d]))
        links[d][i].start()

    sq[...] = jnp.zeros_like(sq)
    for k, kind in enumerate(("S1", "S2")):
        for b in range(6):
            for h in range(2):
                r = chip(kind, h)
                ready((kind, b, h))
                add(b, h, r, [part(b, r, h)])
                send(h, 6 * k + b, own(b, r, h), rec(b, h, k))

    def slot(b, h):
        num = half(b, h)[1]
        if b < 4:
            return mv_a.at[h, 0], mv_a.at[h, 1], ws_a.at[h]
        return mv_b.at[h, 0, pl.ds(0, num)], mv_b.at[h, 1, pl.ds(0, num)], ws_b.at[h, pl.ds(0, num)]

    states = {}

    def fetch_state(b, h):
        m, v, w = slot(b, h)
        states[b, h] = [
            pltpu.make_async_copy(mine(ms, b, h), m, wmv_sem.at[b, h, 0]),
            pltpu.make_async_copy(mine(vs, b, h), v, wmv_sem.at[b, h, 1]),
            pltpu.make_async_copy(span(weights, b, h, me), w, wmv_sem.at[b, h, 2]),
        ]
        for one in states[b, h]:
            one.start()

    for b in (0, 4):
        for h in range(2):
            fetch_state(b, h)

    keep = {}

    def finish(b):
        for h in range(2):
            ready(("G", b, h))
            links[h][6 + b].wait_recv()
            links[1 - h][12 + b].wait_recv()
            add(b, h, 0, [part(b, 0, h), rec(b, h, 1), rec(b, h, 2)], squares=True)
            keep[b, h] = pltpu.make_async_copy(own(b, 0, h), mine(qs, b, h), g_sem.at[b, h])
            keep[b, h].start()

    for b in range(6):
        for h in range(2):
            r = chip("R", h)
            ready(("R", b, h))
            links[h][b].wait_recv()
            add(b, h, r, [part(b, r, h), rec(b, h, 0)])
            send(1 - h, 12 + b, own(b, r, h), rec(b, h, 2))
        if b >= 2:
            finish(b - 2)
    for b in (4, 5):
        finish(b)

    nrm[me] = sq[0:8] + sq[8:16]
    sums = []
    for k in range(1, N):
        other = lax.rem(me + k, N)
        one = pltpu.make_async_remote_copy(nrm.at[me], nrm.at[me], nrm_send.at[k], nrm_recv.at[me], **to(other))
        one.start()
        sums.append(one)
    for k in range(1, N):
        other = lax.rem(me + k, N)
        pltpu.make_async_remote_copy(nrm.at[other], nrm.at[other], nrm_send.at[k], nrm_recv.at[other], **to(other)).wait_recv()
    total = nrm[0]
    for k in range(1, N):
        total = total + nrm[k]
    total = jnp.full((8, 128), jnp.sum(total), jnp.float32)
    fac[...] = jnp.minimum(1.0, 0.5 * lax.rsqrt(total / COUNT + 1e-30))

    def adamw(b, h):
        for one in states[b, h]:
            one.wait()
        keep[b, h].wait()
        m_ref, v_ref, w_ref = slot(b, h)
        target = own(b, 0, h)

        def body(i, carry):
            at = pl.ds(pl.multiple_of(i * 16, 16), 16)
            for lo, width in columns(b):
                cols = pl.ds(lo, width)
                g = f32(target[at, cols]) * jnp.broadcast_to(fac[0:1, 0:1], (16, width))
                m = 0.9 * m_ref[at, cols] + 0.1 * g
                v = 0.95 * v_ref[at, cols] + 0.05 * g * g
                w = f32(w_ref[at, cols])
                step = m * lax.rsqrt(v + 1e-8) + 0.1 * w
                target[at, cols] = (w - 0.02 * step).astype(jnp.bfloat16)
            return carry

        lax.fori_loop(0, half(b, h)[1] // 16, body, 0)

    gats, moves, locals_ = [{}, {}], [], []

    def gather_send(d, i, src, b, h, dev):
        if i >= WINDOW:
            gats[d][i - WINDOW].wait_send()
        gats[d][i] = pltpu.make_async_remote_copy(
            src, span(outs, b, h, dev), gat_send.at[d, i], gat_recv.at[d, i], **to(across[d]))
        gats[d][i].start()

    def hand_over(i, src, b, h, dev):
        one = pltpu.make_async_remote_copy(src, span(outs, b, h, dev), gd_send.at[i], gd_recv.at[i], **to(partner))
        one.start()
        moves.append(one)

    def arrived(d, i):
        gats[d][i].wait_recv()
        b, h = i % 6, (d if i < 6 else 1 - d)
        dev = across[d] if i < 12 else device(3)
        hand_over(12 + 18 * d + i, span(outs, b, h, dev), b, h, dev)

    for i in range(18):
        b = i % 6
        for d in range(2):
            if i < 6:
                adamw(b, d)
                if b + 1 < 6 and b + 1 != 4:
                    fetch_state(b + 1, d)
                gather_send(d, i, own(b, 0, d), b, d, me)
            elif i < 12:
                gather_send(d, i, own(b, 0, 1 - d), b, 1 - d, me)
            else:
                gather_send(d, i, span(outs, b, 1 - d, across[1 - d]), b, 1 - d, across[1 - d])
        if i < 6:
            for h in range(2):
                hand_over(2 * b + h, own(b, 0, h), b, h, me)
                one = pltpu.make_async_copy(own(b, 0, h), span(outs, b, h, me), out_sem.at[b, h])
                one.start()
                locals_.append(one)
        if i >= WINDOW:
            for d in range(2):
                arrived(d, i - WINDOW)
    for i in (16, 17):
        for d in range(2):
            arrived(d, i)

    for i in range(len(order)):
        d2ds[i].wait_send()
    for d in range(2):
        for i in (16, 17):
            links[d][i].wait_send()
            gats[d][i].wait_send()
    for one in sums:
        one.wait_send()
    for one in locals_:
        one.wait()
    for one in moves:
        one.wait()


def communicate(*arrays):
    bf, fl = jnp.bfloat16, jnp.float32
    any_, dma = pl.BlockSpec(memory_space=pl.ANY), pltpu.SemaphoreType.DMA
    wide, tall = [(LAYERS, D, FF)] * 2 + [(LAYERS, FF, D)], [(LAYERS, D // N, FF)] * 2 + [(LAYERS, FF // N, D)]
    return pl.pallas_call(
        kernel,
        out_shape=[jax.ShapeDtypeStruct(s, bf) for s in wide + tall] + [jax.ShapeDtypeStruct((8, 128), fl)],
        in_specs=[any_] * 12,
        out_specs=[any_] * 6 + [pl.BlockSpec(memory_space=pltpu.VMEM)],
        scratch_shapes=[
            pltpu.VMEM((4, 4, 128, 3200), bf), pltpu.VMEM((2, 4, 400, 1024), bf),
            pltpu.VMEM((4, 4, 128, 3200), bf), pltpu.VMEM((2, 4, 400, 1024), bf),
            pltpu.VMEM((4, 2, 3, 64, 3200), bf), pltpu.VMEM((2, 2, 3, 208, 1024), bf),
            pltpu.VMEM((2, 2, 64, 3200), fl), pltpu.VMEM((2, 2, 208, 1024), fl),
            pltpu.VMEM((2, 64, 3200), bf), pltpu.VMEM((2, 208, 1024), bf),
            pltpu.VMEM((16, 128), fl), pltpu.VMEM((8, 8, 128), fl),
            dma((48,)), dma((48,)), dma((48,)), dma((2, 18)), dma((2, 18)), dma((8,)), dma((8,)),
            dma((2, 18)), dma((2, 18)), dma((48,)), dma((48,)), dma((6, 2, 3)), dma((6, 2)), dma((6, 2)),
        ],
        compiler_params=pltpu.CompilerParams(collective_id=0, has_side_effects=True, vmem_limit_bytes=67043328),
    )(*arrays)


def solution(mesh):
    def step(*arrays):
        *out, factor = communicate(*arrays)
        m, v = arrays[6:9], arrays[9:12]
        factor = factor[0, 0]
        g = [q.astype(jnp.float32) * factor for q in out[3:6]]
        return (*out[:3], *(0.9 * a + 0.1 * b for a, b in zip(m, g, strict=True)), *(0.95 * a + 0.05 * b * b for a, b in zip(v, g, strict=True)))

    all_of, cut = P(None, None, None), P(None, "dp", None)
    return jax.shard_map(
        step,
        mesh=mesh,
        in_specs=(P(("rep", "dp"), None, None, None),) * 3 + (all_of,) * 3 + (cut,) * 6,
        out_specs=(P("rep", None, None),) * 3 + (P("rep", "dp", None),) * 6,
        check_vma=False,
    )
```

```python
import functools

import jax
import jax.numpy as jnp
from jax import lax
from jax.experimental import pallas as pl
from jax.experimental.pallas import tpu as pltpu
from jax.sharding import PartitionSpec as P


D, FF, LAYERS, N = 1024, 3200, 2, 8
COUNT = 3 * LAYERS * D * FF
BLOCKS = ((0, 0), (0, 1), (1, 0), (1, 1), (2, 0), (2, 1))
AHEAD = 8
DEPTH = 8
WINDOW = 2


def rows_of(b):
    return 128 if b < 4 else 400


def half(b, h):
    rows = rows_of(b)
    split = 64 if b < 4 else (208 if b == 4 else 192)
    return (0, split) if h == 0 else (split, rows - split)


def columns(b):
    return [(i * 640, 640) for i in range(5)] if b < 4 else [(i * 512, 512) for i in range(2)]


def f32(x):
    return x.astype(jnp.float32)


def kernel(gg, gu, gd, wg, wu, wd, mg, mu, md, vg, vu, vd,
           og, ou, od, qg, qu, qd, fac, *rest):
    *passed, \
        own_a, own_b, part_a, part_b, rec_a, rec_b, mv_a, mv_b, ws_a, ws_b, sq, nrm, \
        load_sem, d2d_send, d2d_recv, link_send, link_recv, nrm_send, nrm_recv, \
        gat_send, gat_recv, gd_send, gd_recv, wmv_sem, out_sem, g_sem = rest
    grads, weights, ms, vs, outs, qs = (gg, gu, gd), (wg, wu, wd), (mg, mu, md), (vg, vu, vd), (og, ou, od), (qg, qu, qd)
    me = lax.axis_index("dp")
    x, y, c = lax.div(me, 4), lax.rem(lax.div(me, 2), 2), lax.rem(me, 2)

    def device(r, other=0):
        cx, cy = lax.rem(x + r // 2, 2), lax.rem(y + r % 2, 2)
        return cx * 4 + cy * 2 + (1 - c if other else c)

    def to(index):
        return dict(device_id={"dp": index}, device_id_type=pl.DeviceIdType.MESH)

    across = (device(2), device(1))
    partner = device(0, 1)

    def own(b, r, h):
        lo, num = half(b, h)
        return (own_a.at[b, r, pl.ds(lo, num)] if b < 4 else own_b.at[b - 4, r, pl.ds(lo, num)])

    def part(b, r, h):
        lo, num = half(b, h)
        return (part_a.at[b, r, pl.ds(lo, num)] if b < 4 else part_b.at[b - 4, r, pl.ds(lo, num)])

    def rec(b, h, k):
        _, num = half(b, h)
        return (rec_a.at[b, h, k] if b < 4 else rec_b.at[b - 4, h, k, pl.ds(0, num)])

    def span(ref, b, h, dev, lead=()):
        lo, num = half(b, h)
        w, layer = BLOCKS[b]
        return ref[w].at[(*lead, layer, pl.ds(pl.multiple_of(dev * rows_of(b) + lo, 16), num))]

    def mine(ref, b, h):
        lo, num = half(b, h)
        return ref[BLOCKS[b][0]].at[BLOCKS[b][1], pl.ds(lo, num)]

    barrier = pltpu.get_barrier_semaphore()
    for k in range(1, N):
        pl.semaphore_signal(barrier, inc=1, **to(lax.rem(me + k, N)))

    def chip(kind, h):
        return {"S1": 3, "S2": (2, 1)[h], "R": (1, 2)[h], "G": 0}[kind]

    order = [(kind, b, h) for kind in ("S1", "S2", "R", "G") for b in range(6) for h in range(2)]
    place = {step: i for i, step in enumerate(order)}
    loads, d2ds = {}, {}

    def fetch_own(i):
        kind, b, h = order[i]
        r = chip(kind, h)
        loads[i] = pltpu.make_async_copy(span(grads, b, h, device(r), (0,)), own(b, r, h), load_sem.at[i])
        loads[i].start()

    def fetch_part(i):
        kind, b, h = order[i]
        r = chip(kind, h)
        d2ds[i] = pltpu.make_async_remote_copy(
            span(grads, b, h, device(r, 1), (0,)), part(b, r, h), d2d_send.at[i], d2d_recv.at[i], **to(partner))
        d2ds[i].start()

    for i in range(AHEAD):
        fetch_own(i)
    pl.semaphore_wait(barrier, N - 1)
    for i in range(AHEAD):
        fetch_part(i)

    def ready(step):
        i = place[step]
        if i + AHEAD < len(order):
            fetch_own(i + AHEAD)
            fetch_part(i + AHEAD)
        loads[i].wait()
        d2ds[i].wait_recv()

    def add(b, h, r, terms, squares=False):
        num = half(b, h)[1]
        target = own(b, r, h)

        def body(i, carry):
            at = pl.ds(pl.multiple_of(i * 16, 16), 16)
            for lo, width in columns(b):
                total = f32(target[at, pl.ds(lo, width)])
                for t in terms:
                    total = total + f32(t[at, pl.ds(lo, width)])
                rounded = total.astype(jnp.bfloat16)
                target[at, pl.ds(lo, width)] = rounded
                if squares:
                    g = f32(rounded)
                    g = g * g
                    s = g[:, 0:128]
                    for k in range(1, width // 128):
                        s = s + g[:, k * 128:(k + 1) * 128]
                    carry = carry + s
            return carry

        done = lax.fori_loop(0, num // 16, body, jnp.zeros((16, 128), jnp.float32) if squares else 0)
        if squares:
            sq[...] += done

    links = [{}, {}]

    def send(d, i, src, dst):
        if i >= WINDOW:
            links[d][i - WINDOW].wait_send()
        links[d][i] = pltpu.make_async_remote_copy(src, dst, link_send.at[d, i], link_recv.at[d, i], **to(across[d]))
        links[d][i].start()

    sq[...] = jnp.zeros_like(sq)
    for k, kind in enumerate(("S1", "S2")):
        for b in range(6):
            for h in range(2):
                r = chip(kind, h)
                ready((kind, b, h))
                add(b, h, r, [part(b, r, h)])
                send(h, 6 * k + b, own(b, r, h), rec(b, h, k))

    def slot(b, h):
        num = half(b, h)[1]
        if b < 4:
            return mv_a.at[h, 0], mv_a.at[h, 1], ws_a.at[h]
        return mv_b.at[h, 0, pl.ds(0, num)], mv_b.at[h, 1, pl.ds(0, num)], ws_b.at[h, pl.ds(0, num)]

    states = {}

    def fetch_state(b, h):
        m, v, w = slot(b, h)
        states[b, h] = [
            pltpu.make_async_copy(mine(ms, b, h), m, wmv_sem.at[b, h, 0]),
            pltpu.make_async_copy(mine(vs, b, h), v, wmv_sem.at[b, h, 1]),
            pltpu.make_async_copy(span(weights, b, h, me), w, wmv_sem.at[b, h, 2]),
        ]
        for one in states[b, h]:
            one.start()

    for b in (0, 4):
        for h in range(2):
            fetch_state(b, h)

    keep = {}

    def finish(b):
        for h in range(2):
            ready(("G", b, h))
            links[h][6 + b].wait_recv()
            links[1 - h][12 + b].wait_recv()
            add(b, h, 0, [part(b, 0, h), rec(b, h, 1), rec(b, h, 2)], squares=True)
            keep[b, h] = pltpu.make_async_copy(own(b, 0, h), mine(qs, b, h), g_sem.at[b, h])
            keep[b, h].start()

    for b in range(6):
        for h in range(2):
            r = chip("R", h)
            ready(("R", b, h))
            links[h][b].wait_recv()
            add(b, h, r, [part(b, r, h), rec(b, h, 0)])
            send(1 - h, 12 + b, own(b, r, h), rec(b, h, 2))
        if b >= 2:
            finish(b - 2)
    for b in (4, 5):
        finish(b)

    nrm[me] = sq[0:8] + sq[8:16]
    sums = []
    for k in range(1, N):
        other = lax.rem(me + k, N)
        one = pltpu.make_async_remote_copy(nrm.at[me], nrm.at[me], nrm_send.at[k], nrm_recv.at[me], **to(other))
        one.start()
        sums.append(one)
    for k in range(1, N):
        other = lax.rem(me + k, N)
        pltpu.make_async_remote_copy(nrm.at[other], nrm.at[other], nrm_send.at[k], nrm_recv.at[other], **to(other)).wait_recv()
    total = nrm[0]
    for k in range(1, N):
        total = total + nrm[k]
    total = jnp.full((8, 128), jnp.sum(total), jnp.float32)
    fac[...] = jnp.minimum(1.0, 0.5 * lax.rsqrt(total / COUNT + 1e-30))

    def adamw(b, h):
        for one in states[b, h]:
            one.wait()
        keep[b, h].wait()
        m_ref, v_ref, w_ref = slot(b, h)
        target = own(b, 0, h)

        def body(i, carry):
            at = pl.ds(pl.multiple_of(i * 16, 16), 16)
            for lo, width in columns(b):
                cols = pl.ds(lo, width)
                g = f32(target[at, cols]) * jnp.broadcast_to(fac[0:1, 0:1], (16, width))
                m = 0.9 * m_ref[at, cols] + 0.1 * g
                v = 0.95 * v_ref[at, cols] + 0.05 * g * g
                w = f32(w_ref[at, cols])
                step = m * lax.rsqrt(v + 1e-8) + 0.1 * w
                target[at, cols] = (w - 0.02 * step).astype(jnp.bfloat16)
            return carry

        lax.fori_loop(0, half(b, h)[1] // 16, body, 0)

    gats, moves, locals_ = [{}, {}], [], []

    def landing(b, h, d, dev):
        if h == d:
            ref = passed[4 * d + min(b // 2, 2) + (b == 5)]
            return ref.at[BLOCKS[b][1]] if b < 4 else ref
        return span(outs, b, h, dev)

    def gather_send(d, i, src, b, h):
        if i >= WINDOW:
            gats[d][i - WINDOW].wait_send()
        gats[d][i] = pltpu.make_async_remote_copy(
            src, landing(b, h, d, me), gat_send.at[d, i], gat_recv.at[d, i], **to(across[d]))
        gats[d][i].start()

    def hand_over(i, src, b, h, dev):
        one = pltpu.make_async_remote_copy(src, span(outs, b, h, dev), gd_send.at[i], gd_recv.at[i], **to(partner))
        one.start()
        moves.append(one)

    def arrived(d, i):
        gats[d][i].wait_recv()
        b, h = i % 6, (d if i < 6 else 1 - d)
        hand_over(12 + 12 * d + i, landing(b, h, d, across[d]), b, h, across[d])

    for i in range(12):
        b = i % 6
        for d in range(2):
            h = d if i < 6 else 1 - d
            if i < 6:
                adamw(b, d)
                if b + 1 < 6 and b + 1 != 4:
                    fetch_state(b + 1, d)
            gather_send(d, i, own(b, 0, h), b, h)
        if i < 6:
            for h in range(2):
                hand_over(2 * b + h, own(b, 0, h), b, h, me)
                one = pltpu.make_async_copy(own(b, 0, h), span(outs, b, h, me), out_sem.at[b, h])
                one.start()
                locals_.append(one)
        if i >= WINDOW:
            for d in range(2):
                arrived(d, i - WINDOW)
    for i in (10, 11):
        for d in range(2):
            arrived(d, i)

    for i in range(len(order)):
        d2ds[i].wait_send()
    for d in range(2):
        for i in (16, 17):
            links[d][i].wait_send()
        for i in (10, 11):
            gats[d][i].wait_send()
    for one in sums:
        one.wait_send()
    for one in locals_:
        one.wait()
    for one in moves:
        one.wait()


def onward(h):
    return [(2, 64, 3200), (2, 64, 3200), (half(4, h)[1], 1024), (half(5, h)[1], 1024)]


def communicate(*arrays):
    bf, fl = jnp.bfloat16, jnp.float32
    any_, dma = pl.BlockSpec(memory_space=pl.ANY), pltpu.SemaphoreType.DMA
    wide, tall = [(LAYERS, D, FF)] * 2 + [(LAYERS, FF, D)], [(LAYERS, D // N, FF)] * 2 + [(LAYERS, FF // N, D)]
    return pl.pallas_call(
        kernel,
        out_shape=[jax.ShapeDtypeStruct(s, bf) for s in wide + tall] + [jax.ShapeDtypeStruct((8, 128), fl)]
        + [jax.ShapeDtypeStruct(s, bf) for s in onward(0) + onward(1)],
        in_specs=[any_] * 12,
        out_specs=[any_] * 6 + [pl.BlockSpec(memory_space=pltpu.VMEM)] + [any_] * 8,
        scratch_shapes=[
            pltpu.VMEM((4, 4, 128, 3200), bf), pltpu.VMEM((2, 4, 400, 1024), bf),
            pltpu.VMEM((4, 4, 128, 3200), bf), pltpu.VMEM((2, 4, 400, 1024), bf),
            pltpu.VMEM((4, 2, 3, 64, 3200), bf), pltpu.VMEM((2, 2, 3, 208, 1024), bf),
            pltpu.VMEM((2, 2, 64, 3200), fl), pltpu.VMEM((2, 2, 208, 1024), fl),
            pltpu.VMEM((2, 64, 3200), bf), pltpu.VMEM((2, 208, 1024), bf),
            pltpu.VMEM((16, 128), fl), pltpu.VMEM((8, 8, 128), fl),
            dma((48,)), dma((48,)), dma((48,)), dma((2, 18)), dma((2, 18)), dma((8,)), dma((8,)),
            dma((2, 12)), dma((2, 12)), dma((36,)), dma((36,)), dma((6, 2, 3)), dma((6, 2)), dma((6, 2)),
        ],
        compiler_params=pltpu.CompilerParams(collective_id=0, has_side_effects=True, vmem_limit_bytes=67043328),
    )(*arrays)


def stream(pieces, slots, sem, depth):
    n, count = len(pieces), slots.shape[0]
    loads = [pltpu.make_async_copy(src, slots.at[i % count, pl.ds(0, src.shape[0])], sem.at[0, i % count]) for i, (src, _) in enumerate(pieces)]
    stores = [pltpu.make_async_copy(slots.at[i % count, pl.ds(0, dst.shape[0])], dst, sem.at[1, i % count]) for i, (_, dst) in enumerate(pieces)]
    for i in range(n + depth):
        if i < n:
            if i >= count:
                stores[i - count].wait()
            loads[i].start()
        if i >= depth:
            loads[i - depth].wait()
            stores[i - depth].start()
    for one in stores[max(0, n - count):]:
        one.wait()


def device_of(r, other):
    me = lax.axis_index("dp")
    x, y, c = lax.div(me, 4), lax.rem(lax.div(me, 2), 2), lax.rem(me, 2)
    return lax.rem(x + r // 2, 2) * 4 + lax.rem(y + r % 2, 2) * 2 + (1 - c if other else c)


def rows(ref, b, dev, lo, num):
    return ref.at[BLOCKS[b][1], pl.ds(pl.multiple_of(dev * rows_of(b) + lo, 16), num)]


def settle_kernel(*refs):
    tmps, passed, qs, fac, ms, vs = refs[:3], (refs[3:7], refs[7:11]), refs[11:14], refs[14], refs[15:18], refs[18:21]
    outs, new_ms, new_vs = refs[21:24], refs[24:27], refs[27:30]
    wide, tall, mv_a, mv_b, g_a, g_b, c_sem, m_sem = refs[30:]

    copies, moments = [], []
    for b in range(6):
        w, layer = BLOCKS[b]
        for r in (0, 1, 2):
            for other in (0, 1):
                dev = device_of(r, other)
                if r == 0 or other:
                    copies.append((b, rows(tmps[w], b, dev, 0, rows_of(b)), rows(outs[w], b, dev, 0, rows_of(b))))
                    continue
                for h in range(2):
                    lo, num = half(b, h)
                    src = rows(tmps[w], b, dev, lo, num)
                    if h == 2 - r:
                        src = passed[h][w].at[layer] if b < 4 else passed[h][b - 2]
                    copies.append((b, src, rows(outs[w], b, dev, lo, num)))
        moments += [(b, h) for h in range(2)]

    loads, stores, work, users = [], [], [], []
    counts = {}

    def take(kind, slots):
        k = counts.get(kind, 0)
        counts[kind] = k + 1
        return k % slots

    def copy_task(b, src, dst):
        kind, ref, base = ("wide", wide, 0) if b < 4 else ("tall", tall, wide.shape[0])
        k = take(kind, ref.shape[0])
        mid = ref.at[k, pl.ds(0, src.shape[0])]
        loads.append([pltpu.make_async_copy(src, mid, c_sem.at[0, base + k])])
        stores.append([pltpu.make_async_copy(mid, dst, c_sem.at[1, base + k])])
        work.append(None)
        users.append((kind, k))

    def moment_task(b, h):
        kind, mv, gs, base = ("a", mv_a, g_a, 0) if b < 4 else ("b", mv_b, g_b, mv_a.shape[0])
        k = take(kind, mv.shape[0])
        w, layer = BLOCKS[b]
        lo, num = half(b, h)
        m, v, g = mv.at[k, 0, pl.ds(0, num)], mv.at[k, 1, pl.ds(0, num)], gs.at[k, pl.ds(0, num)]

        def at(refs_):
            return refs_[w].at[layer, pl.ds(lo, num)]

        loads.append([pltpu.make_async_copy(at(x), y, m_sem.at[i, base + k]) for i, (x, y) in enumerate(((ms, m), (vs, v), (qs, g)))])
        stores.append([pltpu.make_async_copy(y, at(x), m_sem.at[3 + i, base + k]) for i, (x, y) in enumerate(((new_ms, m), (new_vs, v)))])
        users.append((kind, k))

        def compute():
            def body(i, carry):
                some = pl.ds(pl.multiple_of(i * 16, 16), 16)
                for first, width in columns(b):
                    cols = pl.ds(first, width)
                    one = f32(g[some, cols]) * jnp.broadcast_to(fac[0:1, 0:1], (16, width))
                    m[some, cols] = 0.9 * m[some, cols] + 0.1 * one
                    v[some, cols] = 0.95 * v[some, cols] + 0.05 * one * one
                return carry

            lax.fori_loop(0, num // 16, body, 0)

        work.append(compute)

    every = len(copies) / len(moments)
    done = 0
    for i, one in enumerate(copies):
        copy_task(*one)
        while done < len(moments) and (done + 0.5) * every <= i + 1:
            moment_task(*moments[done])
            done += 1

    last = {}
    for i in range(len(users) + DEPTH):
        if i < len(users):
            if users[i] in last:
                for one in stores[last[users[i]]]:
                    one.wait()
            last[users[i]] = i
            for one in loads[i]:
                one.start()
        if i >= DEPTH:
            for one in loads[i - DEPTH]:
                one.wait()
            if work[i - DEPTH] is not None:
                work[i - DEPTH]()
            for one in stores[i - DEPTH]:
                one.start()
    for i in last.values():
        for one in stores[i]:
            one.wait()


def settle(*operands):
    bf, fl = jnp.bfloat16, jnp.float32
    any_, dma = pl.BlockSpec(memory_space=pl.ANY), pltpu.SemaphoreType.DMA
    return pl.pallas_call(
        settle_kernel,
        out_shape=[jax.ShapeDtypeStruct(x.shape, x.dtype) for x in (*operands[:3], *operands[15:21])],
        in_specs=[any_] * 14 + [pl.BlockSpec(memory_space=pltpu.VMEM)] + [any_] * 6,
        out_specs=[any_] * 9,
        scratch_shapes=[
            pltpu.VMEM((16, 128, 3200), bf), pltpu.VMEM((10, 400, 1024), bf),
            pltpu.VMEM((4, 2, 64, 3200), fl), pltpu.VMEM((4, 2, 208, 1024), fl),
            pltpu.VMEM((4, 64, 3200), bf), pltpu.VMEM((4, 208, 1024), bf),
            dma((2, 26)), dma((5, 8)),
        ],
        cost_estimate=pl.CostEstimate(flops=3 * 10**10, bytes_accessed=103 * 10**6, transcendentals=0),
        compiler_params=pltpu.CompilerParams(vmem_limit_bytes=67043328),
    )(*operands)


def far_kernel(blocks, old, *rest):
    *got, out, slots, sem = rest
    pieces = []
    for b in blocks:
        for other in (0, 1):
            for h in range(2):
                lo, num = half(b, h)
                src = got[2 * other + h]
                pieces.append((src.at[BLOCKS[b][1]] if b < 4 else src, rows(out, b, device_of(3, other), lo, num)))
    stream(pieces, slots, sem, len(pieces))


def plain(body, shape, operands, slots, piece, flops, aliases):
    any_ = pl.BlockSpec(memory_space=pl.ANY)
    return pl.pallas_call(
        body,
        out_shape=jax.ShapeDtypeStruct(shape, jnp.bfloat16),
        in_specs=[any_] * len(operands),
        out_specs=any_,
        scratch_shapes=[pltpu.VMEM((slots, *piece), jnp.bfloat16), pltpu.SemaphoreType.DMA((2, slots))],
        input_output_aliases=aliases,
        cost_estimate=pl.CostEstimate(flops=flops, bytes_accessed=slots * piece[0] * piece[1] * 4, transcendentals=0),
        compiler_params=pltpu.CompilerParams(vmem_limit_bytes=67043328),
    )(*operands)


def solution(mesh):
    swap = [[(i, i ^ bit) for i in range(N)] for bit in (4, 2, 1)]
    stages = ((0, 1), (2, 3), (4,), (5,))

    def move(array, pairs):
        return lax.ppermute(array, "dp", pairs)

    def step(*arrays):
        out = communicate(*arrays)
        tmp, q, factor, ahead = out[:3], out[3:6], out[6], (out[7:11], out[11:15])
        first = [[move(ahead[h][s], swap[1 - h]) for h in range(2)] for s in range(len(stages))]
        second = [[move(one, swap[2]) for one in stage] for stage in first]
        done = settle(*tmp, *ahead[0], *ahead[1], *q, factor, *arrays[6:12])
        whole = list(done[:3])
        for s, blocks in enumerate(stages):
            w = min(s, 2)
            piece = (64, 3200) if w < 2 else (208, 1024)
            operands = (whole[w], *first[s], *second[s])
            whole[w] = plain(functools.partial(far_kernel, blocks), tmp[w].shape, operands, 4 * len(blocks), piece, 10**8, {0: 0})
        return (*whole, *done[3:])

    all_of, cut = P(None, None, None), P(None, "dp", None)
    return jax.shard_map(
        step,
        mesh=mesh,
        in_specs=(P(("rep", "dp"), None, None, None),) * 3 + (all_of,) * 3 + (cut,) * 6,
        out_specs=(P("rep", None, None),) * 3 + (P("rep", "dp", None),) * 6,
        check_vma=False,
    )
```

```python
import functools

import jax
import jax.numpy as jnp
from jax import lax
from jax.experimental import pallas as pl
from jax.experimental.pallas import tpu as pltpu
from jax.sharding import PartitionSpec as P


D, FF, LAYERS, N = 1024, 3200, 2, 8
COUNT = 3 * LAYERS * D * FF
BLOCKS = ((0, 0), (0, 1), (1, 0), (1, 1), (2, 0), (2, 1))
LAST = 96
FIRST = 32
AHEAD = 6
RING = 4
VMEM = 67043328
BF, FL = jnp.bfloat16, jnp.float32
HALVES = (0, 1)
LANES, PACK = 128, 16
TILE = (8, LANES)
WIDE, TALL, HALF_WIDE, HALF_TALL = (128, 3200), (400, 1024), (64, 3200), (208, 1024)
DEPTH = 8
WINDOW = 2


def rows_of(b):
    return (WIDE if b < 4 else TALL)[0]


def half(b, h):
    rows = rows_of(b)
    split = rows // 2 if b < 4 else rows // 2 + (8 if b == 4 else -8)
    return (split, rows - split) if h else (0, split)


def tiles(b, num, body, carry):
    full, width = (WIDE[1], 640) if b < 4 else (TALL[1], 512)

    def one(i, carry):
        at = pl.ds(pl.multiple_of(i * PACK, PACK), PACK)
        for first in range(0, full, width):
            carry = body(at, pl.ds(first, width), width, carry)
        return carry

    return lax.fori_loop(0, num // PACK, one, carry)


def fold(x):
    return sum(x[:, k:k + LANES] for k in range(0, x.shape[1], LANES))


def f32(x):
    return x.astype(FL)


def passed_on(h):
    n4, n5, (l4, l5) = half(4, h)[1], half(5, h)[1], (half(4, h)[0], half(5, h)[0])
    lo, num = half(0, h)
    table = [(0, 0, 0, lo, FIRST), (1, 0, 0, lo + FIRST, num - FIRST)]
    table += [(1, num * b - FIRST, b, half(b, h)[0], num) for b in (1, 2, 3)]
    return table + [(2, 0, 4, l4, n4), (2, n4, 5, l5, n5 - LAST), (3, 0, 5, l5 + n5 - LAST, LAST)]


def kernel(gg, gu, gd, wg, wu, wd, mg, mu, md, vg, vu, vd,
           og, ou, od, qg, qu, qd, fac_out, *rest):
    pass_x, pass_y, land_x, land_y, \
        own_a, own_b, part_a, part_b, rec_a, rec_b, mv_a, mv_b, ws_a, ws_b, sq, nrm, \
        fac, load_sem, d2d_send, d2d_recv, link_send, link_recv, nrm_send, nrm_recv, \
        wmv_sem, out_sem, g_sem, fac_sem = (rest[0:4], rest[4:8], *rest[8:])
    grads, weights, ms, vs, outs, qs = (gg, gu, gd), (wg, wu, wd), (mg, mu, md), (vg, vu, vd), (og, ou, od), (qg, qu, qd)
    me = lax.axis_index("dp")
    x, y, c = lax.div(me, 4), lax.rem(lax.div(me, 2), 2), lax.rem(me, 2)

    def device(r, other=0):
        cx, cy = lax.rem(x + r // 2, 2), lax.rem(y + r % 2, 2)
        return cx * 4 + cy * 2 + (1 - c if other else c)

    def to(index):
        return dict(device_id={"dp": index}, device_id_type=pl.DeviceIdType.MESH)

    across = (device(2), device(1))
    partner = device(0, 1)

    def own(p, r):
        b, _, lo, num = p
        return own_a.at[b, r, pl.ds(lo, num)] if b < 4 else own_b.at[b - 4, r, pl.ds(lo, num)]

    def part(p, r):
        b, _, lo, num = p
        return part_a.at[b, r, pl.ds(lo, num)] if b < 4 else part_b.at[b - 4, r, pl.ds(lo, num)]

    def rec(p, k):
        b, h, lo, num = p
        at = pl.ds(lo - half(b, h)[0], num)
        return rec_a.at[b, h, k, at] if b < 4 else rec_b.at[b - 4, h, k, at]

    def span(ref, p, dev, lead=()):
        b, _, lo, num = p
        w, layer = BLOCKS[b]
        return ref[w].at[(*lead, layer, pl.ds(pl.multiple_of(dev * rows_of(b) + lo, PACK), num))]

    def mine(ref, p):
        b, _, lo, num = p
        return ref[BLOCKS[b][0]].at[BLOCKS[b][1], pl.ds(lo, num)]

    def cut(b, h, *firsts):
        lo, num = half(b, h)
        found = []
        for n in (*firsts, num - sum(firsts)):
            found.append((b, h, lo, n))
            lo += n
        return found

    barrier = pltpu.get_barrier_semaphore()
    for k in range(1, N):
        pl.semaphore_signal(barrier, inc=1, **to(lax.rem(me + k, N)))

    def chip(kind, h):
        return {"S1": 3, "S2": (2, 1)[h], "R": (1, 2)[h], "G": 0}[kind]

    pieces = {}
    for h in HALVES:
        pieces["S1", h] = [p for b in range(6) for p in (cut(b, h, 16) if b == 0 else cut(b, h))]
        pieces["S2", h] = [p for b in range(6) for p in cut(b, h)]
        pieces["R", h] = pieces["G", h] = [p for b in range(6) for p in (cut(b, h, half(b, h)[1] - 48) if b == 5 else cut(b, h))]
    pairs = {kind: list(zip(pieces[kind, 0], pieces[kind, 1], strict=True)) for kind in ("S1", "S2", "R", "G")}
    turns = [("S1", pair) for pair in pairs["S1"]] + [("S2", pair) for pair in pairs["S2"]]
    for n in range(len(pairs["R"]) + 2):
        turns += [("R", pair) for pair in pairs["R"][n:n + 1]] + [("G", pair) for pair in pairs["G"][n - 2:n - 1] if n >= 2]
    units = [(p[0], chip("S1", 0), *p[2:]) for pair in pairs["S1"][:2] for p in pair]
    units += [(b, chip("S1", 0), 0, rows_of(b)) for b in range(1, 6)]
    units += [(b, chip("S2", h), 0, rows_of(b)) for b in range(6) for h in HALVES]
    units += [(b, 0, 0, rows_of(b)) for b in range(6)]
    loads, d2ds, here = {}, {}, set()

    def fetch_own(i):
        b, r, lo, num = units[i]
        p = (b, None, lo, num)
        loads[i] = pltpu.make_async_copy(span(grads, p, device(r), (0,)), own(p, r), load_sem.at[i % AHEAD])
        loads[i].start()

    def fetch_part(i):
        b, r, lo, num = units[i]
        p = (b, None, lo, num)
        d2ds[i] = pltpu.make_async_remote_copy(
            span(grads, p, device(r, 1), (0,)), part(p, r), d2d_send.at[i % AHEAD], d2d_recv.at[i], **to(partner))
        d2ds[i].start()

    for i in range(AHEAD):
        fetch_own(i)
    pl.semaphore_wait(barrier, N - 1)
    for i in range(AHEAD):
        fetch_part(i)

    def ready(p, r):
        for i, (b, chip_, lo, num) in enumerate(units):
            if (b, chip_) == (p[0], r) and lo <= p[2] and p[2] + p[3] <= lo + num and i not in here:
                here.add(i)
                loads[i].wait()
                d2ds[i].wait()
                if i + AHEAD < len(units):
                    fetch_own(i + AHEAD)
                    fetch_part(i + AHEAD)

    def add(p, r, terms, squares=False):
        b, _, _, num = p
        target = own(p, r)

        def body(at, cols, width, carry):
            total = f32(target[at, cols])
            for t in terms:
                total = total + f32(t[at, cols])
            rounded = total.astype(BF)
            target[at, cols] = rounded
            return carry + f32(rounded) * f32(rounded) if squares else carry

        width = 640 if b < 4 else 512
        done = tiles(b, num, body, jnp.zeros((PACK, width), FL) if squares else 0)
        if squares:
            sq[...] += fold(done)

    links, arrivals = [[], []], [{}, {}]

    def send(d, p, r, k):
        i = len(links[d])
        if i >= WINDOW:
            links[d][i - WINDOW].wait_send()
        one = pltpu.make_async_remote_copy(own(p, r), rec(p, k), link_send.at[d, i % WINDOW], link_recv.at[d, i], **to(across[d]))
        one.start()
        links[d].append(one)
        arrivals[d][p, k] = one

    sq[...] = jnp.zeros_like(sq)
    for kind, pair in turns:
        if kind in ("S1", "S2"):
            for h, p in enumerate(pair):
                r = chip(kind, h)
                ready(p, r)
                add(p, r, [part(p, r)])
                send(h, p, r, int(kind == "S2"))

    def slot(b, h, lo=0, num=None):
        at = pl.ds(lo, half(b, h)[1] if num is None else num)
        if b < 4:
            return mv_a.at[h, 0, at], mv_a.at[h, 1, at], ws_a.at[h, at]
        return mv_b.at[h, 0, at], mv_b.at[h, 1, at], ws_b.at[h, at]

    states = {}

    def fetch_state(b, h):
        m, v, w = slot(b, h)
        p = cut(b, h)[0]
        states[b, h] = [
            pltpu.make_async_copy(mine(ms, p), m, wmv_sem.at[b // 4, h, 0]),
            pltpu.make_async_copy(mine(vs, p), v, wmv_sem.at[b // 4, h, 1]),
            pltpu.make_async_copy(span(weights, p, me), w, wmv_sem.at[b // 4, h, 2]),
        ]
        for one in states[b, h]:
            one.start()

    for b in (0, 4):
        for h in HALVES:
            fetch_state(b, h)

    keep, waited = {}, set()

    def kept(b):
        if b not in waited:
            waited.add(b)
            keep[b].wait()

    def finish(pair):
        for h, p in enumerate(pair):
            ready(p, 0)
            if (cut(p[0], h)[0], 1) not in waited:
                waited.add((cut(p[0], h)[0], 1))
                arrivals[h][cut(p[0], h)[0], 1].wait_recv()
            arrivals[1 - h][p, 2].wait_recv()
            add(p, 0, [part(p, 0), rec(p, 1), rec(p, 2)], squares=True)
        if pair is pairs["G"][-1] or pair[0][0] != pairs["G"][pairs["G"].index(pair) + 1][0][0]:
            b = pair[0][0]
            if b >= RING:
                kept(b - RING)
            p = (b, None, 0, rows_of(b))
            keep[b] = pltpu.make_async_copy(own(p, 0), mine(qs, p), g_sem.at[b % RING])
            keep[b].start()

    for kind, pair in turns:
        if kind == "G":
            finish(pair)
        elif kind == "R":
            for h, p in enumerate(pair):
                r = chip("R", h)
                ready(p, r)
                for q in pieces["S1", h]:
                    if q[0] == p[0] and (q, 0) not in waited:
                        waited.add((q, 0))
                        arrivals[h][q, 0].wait_recv()
                add(p, r, [part(p, r), rec(p, 0)])
                send(1 - h, p, r, 2)

    nrm[me] = sq[0:8] + sq[8:16]
    sums = []
    for k in range(1, N):
        other = lax.rem(me + k, N)
        one = pltpu.make_async_remote_copy(nrm.at[me], nrm.at[me], nrm_send.at[k], nrm_recv.at[me], **to(other))
        one.start()
        sums.append(one)
    for k in range(1, N):
        other = lax.rem(me + k, N)
        pltpu.make_async_remote_copy(nrm.at[other], nrm.at[other], nrm_send.at[k], nrm_recv.at[other], **to(other)).wait_recv()
    total = nrm[0]
    for k in range(1, N):
        total = total + nrm[k]
    total = jnp.full(TILE, jnp.sum(total), FL)
    fac[...] = jnp.minimum(1.0, 0.5 * lax.rsqrt(total / COUNT + 1e-30))
    fac_copy = pltpu.make_async_copy(fac, fac_out, fac_sem.at[0])
    fac_copy.start()

    def adamw(p):
        b, h, lo, num = p
        if (b, h) not in stepped:
            stepped.add((b, h))
            for one in states[b, h]:
                one.wait()
            kept(b)
        m_ref, v_ref, w_ref = slot(b, h, lo - half(b, h)[0], num)
        target = own(p, 0)

        def body(at, cols, width, carry):
            g = f32(target[at, cols]) * jnp.broadcast_to(fac[0:1, 0:1], (PACK, width))
            m = 0.9 * m_ref[at, cols] + 0.1 * g
            v = 0.95 * v_ref[at, cols] + 0.05 * g * g
            w = f32(w_ref[at, cols])
            step = m * lax.rsqrt(v + 1e-8) + 0.1 * w
            target[at, cols] = (w - 0.02 * step).astype(BF)
            return carry

        tiles(b, num, body, 0)

    stepped = set()
    gats, moves, locals_ = [[], []], [], []
    passes, lands = (pass_x, pass_y), (land_x, land_y)

    def gather_send(d, src, dst, note):
        i = len(gats[d])
        (gats[d][i - WINDOW][0] if i >= WINDOW else links[d][i - WINDOW]).wait_send()
        one = pltpu.make_async_remote_copy(src, dst, link_send.at[d, i % WINDOW], link_recv.at[d, i], **to(across[d]))
        one.start()
        gats[d].append((one, note))

    def hand_over(src, p, dev):
        i = len(moves)
        if i >= AHEAD:
            moves[i - AHEAD].wait_send()
        one = pltpu.make_async_remote_copy(src, span(outs, p, dev), d2d_send.at[i % AHEAD], d2d_recv.at[i], **to(partner))
        one.start()
        moves.append(one)

    def arrived(d, i):
        one, note = gats[d][i]
        one.wait_recv()
        if note is not None:
            ref, p = note
            hand_over(ref, p, across[d])

    def settle_own(b):
        p = (b, None, 0, rows_of(b))
        hand_over(own(p, 0), p, me)
        if b >= RING:
            locals_[b - RING].wait()
        one = pltpu.make_async_copy(own(p, 0), span(outs, p, me), out_sem.at[b % RING])
        one.start()
        locals_.append(one)

    tables = [[(a, row, (b, d, lo, num)) for a, row, b, lo, num in passed_on(d)] for d in HALVES]
    count = len(tables[0])
    for n in range(count + 6):
        for d in HALVES:
            if n < count:
                a, row, p = tables[d][n]
                adamw(p)
                b = p[0]
                if b not in [q[2][0] for q in tables[d][n + 1:]] and b not in (3, 5):
                    fetch_state(b + 1, d)
                ref = passes[d][a].at[pl.ds(row, p[3])]
                gather_send(d, own(p, 0), ref, (ref, p))
            else:
                p = cut(n - count, 1 - d)[0]
                gather_send(d, own(p, 0), span(outs, p, me), (span(outs, p, across[d]), p))
        if n < count and b not in [q[2][0] for q in tables[0][n + 1:]]:
            settle_own(b)
        if n >= WINDOW:
            for d in HALVES:
                arrived(d, n - WINDOW)
    for d in HALVES:
        gather_send(d, passes[1 - d][0], lands[1 - d], None)
    for n in range(count + 4, count + 7):
        for d in HALVES:
            arrived(d, n)

    for d in HALVES:
        for one, _ in gats[d][-WINDOW:]:
            one.wait_send()
    for one in sums:
        one.wait_send()
    for one in locals_[-RING:]:
        one.wait()
    for i, one in enumerate(moves):
        one.wait_recv()
        if i >= len(moves) - AHEAD:
            one.wait_send()
    fac_copy.wait()


ONWARD = [(FIRST, FF), (2 * WIDE[0] - FIRST, FF), (TALL[0] - LAST, D), (LAST, D)]


def communicate(*arrays):
    any_, dma = pl.BlockSpec(memory_space=pl.ANY), pltpu.SemaphoreType.DMA
    wide, tall = [(LAYERS, D, FF)] * 2 + [(LAYERS, FF, D)], [(LAYERS, *WIDE)] * 2 + [(LAYERS, *TALL)]
    shapes = [jax.ShapeDtypeStruct(s, BF) for s in wide + tall] + [jax.ShapeDtypeStruct(TILE, FL)]
    shapes += [jax.ShapeDtypeStruct(s, BF) for s in ONWARD + ONWARD + ONWARD[:1] * 2]
    return pl.pallas_call(
        kernel,
        out_shape=shapes,
        in_specs=[any_] * len(arrays),
        out_specs=[any_] * len(shapes),
        scratch_shapes=[
            *(pltpu.VMEM((4, 4, *WIDE), BF), pltpu.VMEM((2, 4, *TALL), BF)) * 2,
            pltpu.VMEM((4, 2, 3, *HALF_WIDE), BF), pltpu.VMEM((2, 2, 3, *HALF_TALL), BF),
            pltpu.VMEM((2, 2, *HALF_WIDE), FL), pltpu.VMEM((2, 2, *HALF_TALL), FL),
            pltpu.VMEM((2, *HALF_WIDE), BF), pltpu.VMEM((2, *HALF_TALL), BF),
            pltpu.VMEM((PACK, LANES), FL), pltpu.VMEM((N, *TILE), FL), pltpu.VMEM(TILE, FL),
            dma((AHEAD,)), dma((AHEAD,)), dma((34,)), dma((2, WINDOW)), dma((2, 20)), dma((N,)), dma((N,)),
            dma((2, 2, 3)), dma((RING,)), dma((RING,)), dma((1,)),
        ],
        compiler_params=pltpu.CompilerParams(collective_id=0, has_side_effects=True, vmem_limit_bytes=VMEM),
    )(*arrays)


def stream(pieces, slots, sem, depth):
    n, count = len(pieces), slots.shape[0]
    loads = [pltpu.make_async_copy(src, slots.at[i % count, pl.ds(0, src.shape[0])], sem.at[i % count]) for i, (src, _) in enumerate(pieces)]
    stores = [pltpu.make_async_copy(slots.at[i % count, pl.ds(0, dst.shape[0])], dst, sem.at[i % count]) for i, (_, dst) in enumerate(pieces)]
    for i in range(n + depth):
        if i < n:
            if i >= count:
                stores[i - count].wait()
            loads[i].start()
        if i >= depth:
            loads[i - depth].wait()
            stores[i - depth].start()
    for one in stores[max(0, n - count):]:
        one.wait()


def device_of(r, other):
    me = lax.axis_index("dp")
    x, y, c = lax.div(me, 4), lax.rem(lax.div(me, 2), 2), lax.rem(me, 2)
    return lax.rem(x + r // 2, 2) * 4 + lax.rem(y + r % 2, 2) * 2 + (1 - c if other else c)


def rows(ref, b, dev, lo, num):
    return ref.at[BLOCKS[b][1], pl.ds(pl.multiple_of(dev * rows_of(b) + lo, PACK), num)]


def settle_kernel(done, moments, *refs):
    refs = list(refs)
    take = lambda n: [refs.pop(0) for _ in range(n)]
    tmps, passed = dict(zip(done, take(len(done)))), (take(4), take(4))
    qs, fac, ms, vs = (take(3), take(1)[0], take(3), take(3)) if moments else (None,) * 4
    outs = dict(zip(done, take(len(done))))
    new_ms, new_vs = (take(3), take(3)) if moments else (None,) * 2
    wide, tall, mv_a, mv_b, g_a, g_b, factor, c_sem, m_sem, f_sem = refs
    if moments:
        get = pltpu.make_async_copy(fac, factor, f_sem.at[0])
        get.start()

    copies, steps = [], []
    for b in range(6):
        w, _ = BLOCKS[b]
        if moments:
            steps += [(b, h) for h in HALVES]
        if w not in done:
            continue
        for r in (0, 1, 2):
            for other in HALVES:
                dev = device_of(r, other)
                if r == 0 or other:
                    copies.append((b, rows(tmps[w], b, dev, 0, rows_of(b)), rows(outs[w], b, dev, 0, rows_of(b))))
                    continue
                for h in HALVES:
                    if h == r - 1:
                        lo, num = half(b, h)
                        copies.append((b, rows(tmps[w], b, dev, lo, num), rows(outs[w], b, dev, lo, num)))
                    else:
                        copies += [
                            (b, passed[h][a].at[pl.ds(row, num)], rows(outs[w], b, dev, lo, num))
                            for a, row, c, lo, num in passed_on(h) if c == b
                        ]

    loads, stores, work, users = [], [], [], []
    counts = {}

    def place(kind, slots):
        k = counts.get(kind, 0)
        counts[kind] = k + 1
        return k % slots

    def copy_task(b, src, dst):
        kind, ref, base = ("wide", wide, 0) if b < 4 else ("tall", tall, wide.shape[0])
        k = place(kind, ref.shape[0])
        mid = ref.at[k, pl.ds(0, src.shape[0])]
        loads.append([pltpu.make_async_copy(src, mid, c_sem.at[base + k])])
        stores.append([pltpu.make_async_copy(mid, dst, c_sem.at[base + k])])
        work.append(None)
        users.append((kind, k))

    def moment_task(b, h):
        kind, mv, gs, base = ("a", mv_a, g_a, 0) if b < 4 else ("b", mv_b, g_b, mv_a.shape[0])
        k = place(kind, mv.shape[0])
        w, layer = BLOCKS[b]
        lo, num = half(b, h)
        m, v, g = mv.at[k, 0, pl.ds(0, num)], mv.at[k, 1, pl.ds(0, num)], gs.at[k, pl.ds(0, num)]

        def at(refs_):
            return refs_[w].at[layer, pl.ds(lo, num)]

        loads.append([pltpu.make_async_copy(at(x), y, m_sem.at[i, base + k]) for i, (x, y) in enumerate(((ms, m), (vs, v), (qs, g)))])
        stores.append([pltpu.make_async_copy(y, at(x), m_sem.at[i, base + k]) for i, (x, y) in enumerate(((new_ms, m), (new_vs, v)))])
        users.append((kind, k))

        def compute():
            def body(at, cols, width, carry):
                one = f32(g[at, cols]) * jnp.broadcast_to(factor[0:1, 0:1], (PACK, width))
                m[at, cols] = 0.9 * m[at, cols] + 0.1 * one
                v[at, cols] = 0.95 * v[at, cols] + 0.05 * one * one
                return carry

            tiles(b, num, body, 0)

        work.append(compute)

    every = len(copies) / max(len(steps), 1)
    n = 0
    for i, one in enumerate(copies):
        copy_task(*one)
        while n < len(steps) and (n + 0.5) * every <= i + 1:
            moment_task(*steps[n])
            n += 1

    last = {}
    if moments:
        get.wait()
    for i in range(len(users) + DEPTH):
        if i < len(users):
            if users[i] in last:
                for one in stores[last[users[i]]]:
                    one.wait()
            last[users[i]] = i
            for one in loads[i]:
                one.start()
        if 0 <= i - DEPTH < len(users):
            for one in loads[i - DEPTH]:
                one.wait()
            if work[i - DEPTH] is not None:
                work[i - DEPTH]()
            for one in stores[i - DEPTH]:
                one.start()
    for i in last.values():
        for one in stores[i]:
            one.wait()


def settle(done, tmp, passed, moments):
    any_, dma = pl.BlockSpec(memory_space=pl.ANY), pltpu.SemaphoreType.DMA
    operands = [*(tmp[w] for w in done), *passed]
    shapes = [tmp[w] for w in done]
    specs = [any_] * len(operands)
    if moments:
        q, factor, m, v = moments
        operands += [*q, factor, *m, *v]
        specs += [any_] * 10
        shapes += [*m, *v]
    flops = 10**10 * len(done) + (10**10 if moments else 0)
    return pl.pallas_call(
        functools.partial(settle_kernel, done, bool(moments)),
        out_shape=[jax.ShapeDtypeStruct(one.shape, one.dtype) for one in shapes],
        in_specs=specs,
        out_specs=[any_] * len(shapes),
        scratch_shapes=[
            pltpu.VMEM((16, *WIDE), BF), pltpu.VMEM((10, *TALL), BF),
            pltpu.VMEM((5, 2, *HALF_WIDE), FL), pltpu.VMEM((5, 2, *HALF_TALL), FL),
            pltpu.VMEM((5, *HALF_WIDE), BF), pltpu.VMEM((5, *HALF_TALL), BF), pltpu.VMEM(TILE, FL),
            dma((26,)), dma((3, 10) if moments else (1, 1)), dma((1,)),
        ],
        cost_estimate=pl.CostEstimate(flops=flops, bytes_accessed=30 * 10**6, transcendentals=0),
        compiler_params=pltpu.CompilerParams(vmem_limit_bytes=VMEM),
    )(*operands)


def far_kernel(done, arrays, *refs):
    got = refs[len(done):len(done) + 4 * len(arrays)]
    outs, (slots, sem) = dict(zip(done, refs[len(done) + 4 * len(arrays):])), refs[-2:]
    pieces = []
    for i, a in enumerate(arrays):
        for other in HALVES:
            for h in HALVES:
                src = got[4 * i + 2 * other + h]
                for c, row, b, lo, num in passed_on(h):
                    if c == a:
                        pieces.append((src.at[pl.ds(row, num)], rows(outs[BLOCKS[b][0]], b, device_of(3, other), lo, num)))
    stream(pieces, slots, sem, len(pieces))


def far(done, arrays, whole, got):
    any_ = pl.BlockSpec(memory_space=pl.ANY)
    piece, slots = (HALF_WIDE, 20) if 0 in done else (HALF_TALL, 8)
    operands = [*(whole[w] for w in done), *got]
    return pl.pallas_call(
        functools.partial(far_kernel, done, arrays),
        out_shape=[jax.ShapeDtypeStruct(whole[w].shape, BF) for w in done],
        in_specs=[any_] * len(operands),
        out_specs=[any_] * len(done),
        scratch_shapes=[pltpu.VMEM((slots, *piece), BF), pltpu.SemaphoreType.DMA((slots,))],
        input_output_aliases={i: i for i in range(len(done))},
        cost_estimate=pl.CostEstimate(flops=10**8, bytes_accessed=10**6, transcendentals=0),
        compiler_params=pltpu.CompilerParams(vmem_limit_bytes=VMEM),
    )(*operands)


def solution(mesh):
    swap = [[(i, i ^ bit) for i in range(N)] for bit in (4, 2, 1)]

    def move(array, pairs):
        return lax.ppermute(array, "dp", pairs)

    def step(*arrays):
        out = communicate(*arrays)
        tmp, q, factor, ahead, first = out[:3], out[3:6], out[6], (out[7:11], out[11:15]), [out[15:17]]
        for s in (1, 2, 3):
            first.append([move(ahead[h][s], swap[1 - h]) for h in HALVES])
        second = [[move(one, swap[2]) for one in stage] for stage in first]
        got = [[*first[s], *second[s]] for s in range(4)]
        passed = [*ahead[0], *ahead[1]]
        whole = [None] * 3
        whole[0], whole[2], *moments = settle((0, 2), tmp, passed, (q, factor, arrays[6:9], arrays[9:12]))
        (whole[1],) = settle((1,), tmp, passed, None)
        whole[0], whole[1] = far((0, 1), (0, 1), whole, [*got[0], *got[1]])
        (whole[2],) = far((2,), (2,), whole, got[2])
        (whole[2],) = far((2,), (3,), whole, got[3])
        return (*whole, *moments)

    all_of, cut = P(None, None, None), P(None, "dp", None)
    return jax.shard_map(
        step,
        mesh=mesh,
        in_specs=(P(("rep", "dp"), None, None, None),) * 3 + (all_of,) * 3 + (cut,) * 6,
        out_specs=(P("rep", None, None),) * 3 + (P("rep", "dp", None),) * 6,
        check_vma=False,
    )
```

```python
import functools

import jax
import jax.numpy as jnp
from jax import lax
from jax.experimental import pallas as pl
from jax.experimental.pallas import tpu as pltpu
from jax.sharding import PartitionSpec as P


D, FF, LAYERS, N = 1024, 3200, 2, 8
COUNT = 3 * LAYERS * D * FF
BLOCKS = ((0, 0), (0, 1), (1, 0), (1, 1), (2, 0), (2, 1))
NB, DOWN = len(BLOCKS), 4
LAST = 144
FIRST = 16
AHEAD = 6
RING = 4
VMEM = 67043328
BF, FL = jnp.bfloat16, jnp.float32
HALVES = (0, 1)
LANES, PACK = 128, 16
TILE = (8, LANES)
WIDE, TALL, HALF_WIDE, HALF_TALL = (128, 3200), (400, 1024), (64, 3200), (208, 1024)
DEPTH = 8
WINDOW = 2


def rows_of(b):
    return (WIDE if b < DOWN else TALL)[0]


def half(b, h):
    rows = rows_of(b)
    split = rows // 2 if b < DOWN else rows // 2 + (8 if b == 4 else -8)
    return (split, rows - split) if h else (0, split)


def tiles(b, num, body, carry):
    full, width = (WIDE[1], 640) if b < DOWN else (TALL[1], 512)

    def one(i, carry):
        at = pl.ds(pl.multiple_of(i * PACK, PACK), PACK)
        for first in range(0, full, width):
            carry = body(at, pl.ds(first, width), width, carry)
        return carry

    return lax.fori_loop(0, num // PACK, one, carry)


def fold(x):
    return sum(x[:, k:k + LANES] for k in range(0, x.shape[1], LANES))


def f32(x):
    return x.astype(FL)


def passed_on(h):
    n4, n5, (l4, l5) = half(4, h)[1], half(5, h)[1], (half(4, h)[0], half(5, h)[0])
    lo, num = half(0, h)
    table = [(0, 0, 0, lo, FIRST), (1, 0, 0, lo + FIRST, num - FIRST)]
    table += [(1, num * b - FIRST, b, half(b, h)[0], num) for b in (1, 2, 3)]
    return table + [(2, 0, 4, l4, n4), (2, n4, 5, l5, n5 - LAST), (3, 0, 5, l5 + n5 - LAST, LAST)]


def kernel(gg, gu, gd, wg, wu, wd, mg, mu, md, vg, vu, vd,
           og, ou, od, qg, qu, qd, fac_out, *rest):
    pass_x, pass_y, land_x, land_y, \
        own_a, own_b, part_a, part_b, rec_a, rec_b, mv_a, mv_b, ws_a, ws_b, sq, nrm, \
        fac, load_sem, d2d_send, d2d_recv, link_send, link_recv, nrm_send, nrm_recv, \
        wmv_sem, out_sem, g_sem, fac_sem = (rest[0:4], rest[4:8], *rest[8:])
    grads, weights, ms, vs, outs, qs = (gg, gu, gd), (wg, wu, wd), (mg, mu, md), (vg, vu, vd), (og, ou, od), (qg, qu, qd)
    me = lax.axis_index("dp")
    x, y, c = lax.div(me, 4), lax.rem(lax.div(me, 2), 2), lax.rem(me, 2)

    def device(r, other=0):
        cx, cy = lax.rem(x + r // 2, 2), lax.rem(y + r % 2, 2)
        return cx * 4 + cy * 2 + (1 - c if other else c)

    def to(index):
        return dict(device_id={"dp": index}, device_id_type=pl.DeviceIdType.MESH)

    across = (device(2), device(1))
    partner = device(0, 1)

    def own(p, r):
        b, _, lo, num = p
        return own_a.at[b, r, pl.ds(lo, num)] if b < DOWN else own_b.at[b - DOWN, r, pl.ds(lo, num)]

    def part(p, r):
        b, _, lo, num = p
        return part_a.at[b, r, pl.ds(lo, num)] if b < DOWN else part_b.at[b - DOWN, r, pl.ds(lo, num)]

    def rec(p, k):
        b, h, lo, num = p
        at = pl.ds(lo - half(b, h)[0], num)
        return rec_a.at[b, h, k, at] if b < DOWN else rec_b.at[b - DOWN, h, k, at]

    def span(ref, p, dev, lead=()):
        b, _, lo, num = p
        w, layer = BLOCKS[b]
        return ref[w].at[(*lead, layer, pl.ds(pl.multiple_of(dev * rows_of(b) + lo, PACK), num))]

    def mine(ref, p):
        b, _, lo, num = p
        return ref[BLOCKS[b][0]].at[BLOCKS[b][1], pl.ds(lo, num)]

    def cut(b, h, *firsts):
        lo, num = half(b, h)
        found = []
        for n in (*firsts, num - sum(firsts)):
            found.append((b, h, lo, n))
            lo += n
        return found

    barrier = pltpu.get_barrier_semaphore()
    for k in range(1, N):
        pl.semaphore_signal(barrier, inc=1, **to(lax.rem(me + k, N)))

    def chip(kind, h):
        return {"S1": 3, "S2": (2, 1)[h], "R": (1, 2)[h], "G": 0}[kind]

    pieces = {}
    for h in HALVES:
        pieces["S1", h] = [p for b in range(NB) for p in (cut(b, h, 16) if b == 0 else cut(b, h))]
        pieces["S2", h] = [p for b in range(NB) for p in cut(b, h)]
        pieces["R", h] = pieces["G", h] = [p for b in range(NB) for p in (cut(b, h, half(b, h)[1] - 48) if b == 5 else cut(b, h))]
    pairs = {kind: list(zip(pieces[kind, 0], pieces[kind, 1], strict=True)) for kind in ("S1", "S2", "R", "G")}
    turns = [("S1", pair) for pair in pairs["S1"]] + [("S2", pair) for pair in pairs["S2"]]
    for n in range(len(pairs["R"]) + 2):
        turns += [("R", pair) for pair in pairs["R"][n:n + 1]] + [("G", pair) for pair in pairs["G"][n - 2:n - 1] if n >= 2]
    units = [(p[0], chip("S1", 0), *p[2:]) for pair in pairs["S1"][:2] for p in pair]
    units += [(b, chip("S1", 0), 0, rows_of(b)) for b in range(1, NB)]
    units += [(b, chip("S2", h), 0, rows_of(b)) for b in range(NB) for h in HALVES]
    units += [(b, 0, 0, rows_of(b)) for b in range(NB)]
    loads, d2ds, here = {}, {}, set()

    def fetch_own(i):
        b, r, lo, num = units[i]
        p = (b, None, lo, num)
        loads[i] = pltpu.make_async_copy(span(grads, p, device(r), (0,)), own(p, r), load_sem.at[i % AHEAD])
        loads[i].start()

    def fetch_part(i):
        b, r, lo, num = units[i]
        p = (b, None, lo, num)
        d2ds[i] = pltpu.make_async_remote_copy(
            span(grads, p, device(r, 1), (0,)), part(p, r), d2d_send.at[i % AHEAD], d2d_recv.at[i], **to(partner))
        d2ds[i].start()

    for i in range(AHEAD):
        fetch_own(i)
    pl.semaphore_wait(barrier, N - 1)
    for i in range(AHEAD):
        fetch_part(i)

    def ready(p, r):
        for i, (b, chip_, lo, num) in enumerate(units):
            if (b, chip_) == (p[0], r) and lo <= p[2] and p[2] + p[3] <= lo + num and i not in here:
                here.add(i)
                loads[i].wait()
                d2ds[i].wait()
                if i + AHEAD < len(units):
                    fetch_own(i + AHEAD)
                    fetch_part(i + AHEAD)

    def add(p, r, terms, squares=False):
        b, _, _, num = p
        target = own(p, r)

        def body(at, cols, width, carry):
            total = f32(target[at, cols])
            for t in terms:
                total = total + f32(t[at, cols])
            rounded = total.astype(BF)
            target[at, cols] = rounded
            return carry + f32(rounded) * f32(rounded) if squares else carry

        width = 640 if b < DOWN else 512
        done = tiles(b, num, body, jnp.zeros((PACK, width), FL) if squares else 0)
        if squares:
            sq[...] += fold(done)

    links, arrivals = [[], []], [{}, {}]

    def send(d, p, r, k):
        i = len(links[d])
        if i >= WINDOW:
            links[d][i - WINDOW].wait_send()
        one = pltpu.make_async_remote_copy(own(p, r), rec(p, k), link_send.at[d, i % WINDOW], link_recv.at[d, i], **to(across[d]))
        one.start()
        links[d].append(one)
        arrivals[d][p, k] = one

    sq[...] = jnp.zeros_like(sq)
    for kind, pair in turns:
        if kind in ("S1", "S2"):
            for h, p in enumerate(pair):
                r = chip(kind, h)
                ready(p, r)
                add(p, r, [part(p, r)])
                send(h, p, r, int(kind == "S2"))

    def slot(b, h, lo=0, num=None):
        at = pl.ds(lo, half(b, h)[1] if num is None else num)
        if b < DOWN:
            return mv_a.at[h, 0, at], mv_a.at[h, 1, at], ws_a.at[h, at]
        return mv_b.at[h, 0, at], mv_b.at[h, 1, at], ws_b.at[h, at]

    states = {}

    def fetch_state(b, h):
        m, v, w = slot(b, h)
        p = cut(b, h)[0]
        states[b, h] = [
            pltpu.make_async_copy(mine(ms, p), m, wmv_sem.at[b // 4, h, 0]),
            pltpu.make_async_copy(mine(vs, p), v, wmv_sem.at[b // 4, h, 1]),
            pltpu.make_async_copy(span(weights, p, me), w, wmv_sem.at[b // 4, h, 2]),
        ]
        for one in states[b, h]:
            one.start()

    for b in (0, 4):
        for h in HALVES:
            fetch_state(b, h)

    keep, waited = {}, set()

    def kept(b):
        if b not in waited:
            waited.add(b)
            keep[b].wait()

    def finish(pair):
        for h, p in enumerate(pair):
            ready(p, 0)
            if (cut(p[0], h)[0], 1) not in waited:
                waited.add((cut(p[0], h)[0], 1))
                arrivals[h][cut(p[0], h)[0], 1].wait_recv()
            arrivals[1 - h][p, 2].wait_recv()
            add(p, 0, [part(p, 0), rec(p, 1), rec(p, 2)], squares=True)
        if pair is pairs["G"][-1] or pair[0][0] != pairs["G"][pairs["G"].index(pair) + 1][0][0]:
            b = pair[0][0]
            if b >= RING:
                kept(b - RING)
            p = (b, None, 0, rows_of(b))
            keep[b] = pltpu.make_async_copy(own(p, 0), mine(qs, p), g_sem.at[b % RING])
            keep[b].start()

    for kind, pair in turns:
        if kind == "G":
            finish(pair)
        elif kind == "R":
            for h, p in enumerate(pair):
                r = chip("R", h)
                ready(p, r)
                for q in pieces["S1", h]:
                    if q[0] == p[0] and (q, 0) not in waited:
                        waited.add((q, 0))
                        arrivals[h][q, 0].wait_recv()
                add(p, r, [part(p, r), rec(p, 0)])
                send(1 - h, p, r, 2)

    nrm[me] = sq[0:8] + sq[8:16]
    sums = []
    for k in range(1, N):
        other = lax.rem(me + k, N)
        one = pltpu.make_async_remote_copy(nrm.at[me], nrm.at[me], nrm_send.at[k], nrm_recv.at[me], **to(other))
        one.start()
        sums.append(one)
    for k in range(1, N):
        other = lax.rem(me + k, N)
        pltpu.make_async_remote_copy(nrm.at[other], nrm.at[other], nrm_send.at[k], nrm_recv.at[other], **to(other)).wait_recv()
    total = nrm[0]
    for k in range(1, N):
        total = total + nrm[k]
    total = jnp.full(TILE, jnp.sum(total), FL)
    fac[...] = jnp.minimum(1.0, 0.5 * lax.rsqrt(total / COUNT + 1e-30))
    fac_copy = pltpu.make_async_copy(fac, fac_out, fac_sem.at[0])
    fac_copy.start()

    def adamw(p):
        b, h, lo, num = p
        if (b, h) not in stepped:
            stepped.add((b, h))
            for one in states[b, h]:
                one.wait()
            kept(b)
        m_ref, v_ref, w_ref = slot(b, h, lo - half(b, h)[0], num)
        target = own(p, 0)

        def body(at, cols, width, carry):
            g = f32(target[at, cols]) * jnp.broadcast_to(fac[0:1, 0:1], (PACK, width))
            m = 0.9 * m_ref[at, cols] + 0.1 * g
            v = 0.95 * v_ref[at, cols] + 0.05 * g * g
            w = f32(w_ref[at, cols])
            step = m * lax.rsqrt(v + 1e-8) + 0.1 * w
            target[at, cols] = (w - 0.02 * step).astype(BF)
            return carry

        tiles(b, num, body, 0)

    stepped = set()
    gats, moves, locals_ = [[], []], [], []
    passes, lands = (pass_x, pass_y), (land_x, land_y)

    def gather_send(d, src, dst, note):
        i = len(gats[d])
        (gats[d][i - WINDOW][0] if i >= WINDOW else links[d][i - WINDOW]).wait_send()
        one = pltpu.make_async_remote_copy(src, dst, link_send.at[d, i % WINDOW], link_recv.at[d, i], **to(across[d]))
        one.start()
        gats[d].append((one, note))

    def hand_over(src, p, dev):
        i = len(moves)
        if i >= AHEAD:
            moves[i - AHEAD].wait_send()
        one = pltpu.make_async_remote_copy(src, span(outs, p, dev), d2d_send.at[i % AHEAD], d2d_recv.at[i], **to(partner))
        one.start()
        moves.append(one)

    def arrived(d, i):
        one, note = gats[d][i]
        one.wait_recv()
        if note is not None:
            ref, p = note
            hand_over(ref, p, across[d])

    def settle_own(b):
        p = (b, None, 0, rows_of(b))
        hand_over(own(p, 0), p, me)
        if b >= RING:
            locals_[b - RING].wait()
        one = pltpu.make_async_copy(own(p, 0), span(outs, p, me), out_sem.at[b % RING])
        one.start()
        locals_.append(one)

    tables = [[(a, row, (b, d, lo, num)) for a, row, b, lo, num in passed_on(d)] for d in HALVES]
    count = len(tables[0])
    for n in range(count + 6):
        for d in HALVES:
            if n < count:
                a, row, p = tables[d][n]
                adamw(p)
                b = p[0]
                if b not in [q[2][0] for q in tables[d][n + 1:]] and b not in (3, 5):
                    fetch_state(b + 1, d)
                ref = passes[d][a].at[pl.ds(row, p[3])]
                gather_send(d, own(p, 0), ref, (ref, p))
            else:
                p = cut(n - count, 1 - d)[0]
                gather_send(d, own(p, 0), span(outs, p, me), (span(outs, p, across[d]), p))
        if n < count and b not in [q[2][0] for q in tables[0][n + 1:]]:
            settle_own(b)
        if n >= WINDOW:
            for d in HALVES:
                arrived(d, n - WINDOW)
    for d in HALVES:
        gather_send(d, passes[1 - d][0], lands[1 - d], None)
    for n in range(count + 4, count + 7):
        for d in HALVES:
            arrived(d, n)

    for d in HALVES:
        for one, _ in gats[d][-WINDOW:]:
            one.wait_send()
    for one in sums:
        one.wait_send()
    for one in locals_[-RING:]:
        one.wait()
    for i, one in enumerate(moves):
        one.wait_recv()
        if i >= len(moves) - AHEAD:
            one.wait_send()
    fac_copy.wait()


ONWARD = [(FIRST, FF), (2 * WIDE[0] - FIRST, FF), (TALL[0] - LAST, D), (LAST, D)]


def communicate(*arrays):
    any_, dma = pl.BlockSpec(memory_space=pl.ANY), pltpu.SemaphoreType.DMA
    wide, tall = [(LAYERS, D, FF)] * 2 + [(LAYERS, FF, D)], [(LAYERS, *WIDE)] * 2 + [(LAYERS, *TALL)]
    shapes = [jax.ShapeDtypeStruct(s, BF) for s in wide + tall] + [jax.ShapeDtypeStruct(TILE, FL)]
    shapes += [jax.ShapeDtypeStruct(s, BF) for s in ONWARD + ONWARD + ONWARD[:1] * 2]
    return pl.pallas_call(
        kernel,
        out_shape=shapes,
        in_specs=[any_] * len(arrays),
        out_specs=[any_] * len(shapes),
        scratch_shapes=[
            *(pltpu.VMEM((4, 4, *WIDE), BF), pltpu.VMEM((2, 4, *TALL), BF)) * 2,
            pltpu.VMEM((4, 2, 3, *HALF_WIDE), BF), pltpu.VMEM((2, 2, 3, *HALF_TALL), BF),
            pltpu.VMEM((2, 2, *HALF_WIDE), FL), pltpu.VMEM((2, 2, *HALF_TALL), FL),
            pltpu.VMEM((2, *HALF_WIDE), BF), pltpu.VMEM((2, *HALF_TALL), BF),
            pltpu.VMEM((PACK, LANES), FL), pltpu.VMEM((N, *TILE), FL), pltpu.VMEM(TILE, FL),
            dma((AHEAD,)), dma((AHEAD,)), dma((34,)), dma((2, WINDOW)), dma((2, 20)), dma((N,)), dma((N,)),
            dma((2, 2, 3)), dma((RING,)), dma((RING,)), dma((1,)),
        ],
        compiler_params=pltpu.CompilerParams(collective_id=0, has_side_effects=True, vmem_limit_bytes=VMEM),
    )(*arrays)


def stream(pieces, slots, sem, depth):
    n, count = len(pieces), slots.shape[0]
    loads = [pltpu.make_async_copy(src, slots.at[i % count, pl.ds(0, src.shape[0])], sem.at[i % count]) for i, (src, _) in enumerate(pieces)]
    stores = [pltpu.make_async_copy(slots.at[i % count, pl.ds(0, dst.shape[0])], dst, sem.at[i % count]) for i, (_, dst) in enumerate(pieces)]
    for i in range(n + depth):
        if i < n:
            if i >= count:
                stores[i - count].wait()
            loads[i].start()
        if i >= depth:
            loads[i - depth].wait()
            stores[i - depth].start()
    for one in stores[max(0, n - count):]:
        one.wait()


def device_of(r, other):
    me = lax.axis_index("dp")
    x, y, c = lax.div(me, 4), lax.rem(lax.div(me, 2), 2), lax.rem(me, 2)
    return lax.rem(x + r // 2, 2) * 4 + lax.rem(y + r % 2, 2) * 2 + (1 - c if other else c)


def rows(ref, b, dev, lo, num):
    return ref.at[BLOCKS[b][1], pl.ds(pl.multiple_of(dev * rows_of(b) + lo, PACK), num)]


def settle_kernel(done, moments, *refs):
    refs = list(refs)
    take = lambda n: [refs.pop(0) for _ in range(n)]
    tmps, passed = dict(zip(done, take(len(done)))), (take(4), take(4))
    qs, fac, ms, vs = (take(3), take(1)[0], take(3), take(3)) if moments else (None,) * 4
    outs = dict(zip(done, take(len(done))))
    new_ms, new_vs = (take(3), take(3)) if moments else (None,) * 2
    wide, tall, mv_a, mv_b, g_a, g_b, factor, c_sem, m_sem, f_sem = refs
    if moments:
        get = pltpu.make_async_copy(fac, factor, f_sem.at[0])
        get.start()

    copies, steps = [], []
    for b in range(NB):
        w, _ = BLOCKS[b]
        if moments:
            steps += [(b, h) for h in HALVES]
        if w not in done:
            continue
        for r in (0, 1, 2):
            for other in HALVES:
                dev = device_of(r, other)
                if r == 0 or other:
                    copies.append((b, rows(tmps[w], b, dev, 0, rows_of(b)), rows(outs[w], b, dev, 0, rows_of(b))))
                    continue
                for h in HALVES:
                    if h == r - 1:
                        lo, num = half(b, h)
                        copies.append((b, rows(tmps[w], b, dev, lo, num), rows(outs[w], b, dev, lo, num)))
                    else:
                        copies += [
                            (b, passed[h][a].at[pl.ds(row, num)], rows(outs[w], b, dev, lo, num))
                            for a, row, c, lo, num in passed_on(h) if c == b
                        ]

    loads, stores, work, users = [], [], [], []
    counts = {}

    def place(kind, slots):
        k = counts.get(kind, 0)
        counts[kind] = k + 1
        return k % slots

    def copy_task(b, src, dst):
        kind, ref, base = ("wide", wide, 0) if b < DOWN else ("tall", tall, wide.shape[0])
        k = place(kind, ref.shape[0])
        mid = ref.at[k, pl.ds(0, src.shape[0])]
        loads.append([pltpu.make_async_copy(src, mid, c_sem.at[base + k])])
        stores.append([pltpu.make_async_copy(mid, dst, c_sem.at[base + k])])
        work.append(None)
        users.append((kind, k))

    def moment_task(b, h):
        kind, mv, gs, base = ("a", mv_a, g_a, 0) if b < DOWN else ("b", mv_b, g_b, mv_a.shape[0])
        k = place(kind, mv.shape[0])
        w, layer = BLOCKS[b]
        lo, num = half(b, h)
        m, v, g = mv.at[k, 0, pl.ds(0, num)], mv.at[k, 1, pl.ds(0, num)], gs.at[k, pl.ds(0, num)]

        def at(refs_):
            return refs_[w].at[layer, pl.ds(lo, num)]

        loads.append([pltpu.make_async_copy(at(x), y, m_sem.at[i, base + k]) for i, (x, y) in enumerate(((ms, m), (vs, v), (qs, g)))])
        stores.append([pltpu.make_async_copy(y, at(x), m_sem.at[i, base + k]) for i, (x, y) in enumerate(((new_ms, m), (new_vs, v)))])
        users.append((kind, k))

        def compute():
            def body(at, cols, width, carry):
                one = f32(g[at, cols]) * jnp.broadcast_to(factor[0:1, 0:1], (PACK, width))
                m[at, cols] = 0.9 * m[at, cols] + 0.1 * one
                v[at, cols] = 0.95 * v[at, cols] + 0.05 * one * one
                return carry

            tiles(b, num, body, 0)

        work.append(compute)

    every = len(copies) / max(len(steps), 1)
    n = 0
    for i, one in enumerate(copies):
        copy_task(*one)
        while n < len(steps) and (n + 0.5) * every <= i + 1:
            moment_task(*steps[n])
            n += 1

    last = {}
    if moments:
        get.wait()
    for i in range(len(users) + DEPTH):
        if i < len(users):
            if users[i] in last:
                for one in stores[last[users[i]]]:
                    one.wait()
            last[users[i]] = i
            for one in loads[i]:
                one.start()
        if 0 <= i - DEPTH < len(users):
            for one in loads[i - DEPTH]:
                one.wait()
            if work[i - DEPTH] is not None:
                work[i - DEPTH]()
            for one in stores[i - DEPTH]:
                one.start()
    for i in last.values():
        for one in stores[i]:
            one.wait()


def settle(done, tmp, passed, moments):
    any_, dma = pl.BlockSpec(memory_space=pl.ANY), pltpu.SemaphoreType.DMA
    operands = [*(tmp[w] for w in done), *passed]
    shapes = [tmp[w] for w in done]
    specs = [any_] * len(operands)
    if moments:
        q, factor, m, v = moments
        operands += [*q, factor, *m, *v]
        specs += [any_] * 10
        shapes += [*m, *v]
    flops = 10**10 * len(done) + (10**10 if moments else 0)
    return pl.pallas_call(
        functools.partial(settle_kernel, done, bool(moments)),
        out_shape=[jax.ShapeDtypeStruct(one.shape, one.dtype) for one in shapes],
        in_specs=specs,
        out_specs=[any_] * len(shapes),
        scratch_shapes=[
            pltpu.VMEM((16, *WIDE), BF), pltpu.VMEM((10, *TALL), BF),
            pltpu.VMEM((5, 2, *HALF_WIDE), FL), pltpu.VMEM((5, 2, *HALF_TALL), FL),
            pltpu.VMEM((5, *HALF_WIDE), BF), pltpu.VMEM((5, *HALF_TALL), BF), pltpu.VMEM(TILE, FL),
            dma((26,)), dma((3, 10) if moments else (1, 1)), dma((1,)),
        ],
        cost_estimate=pl.CostEstimate(flops=flops, bytes_accessed=30 * 10**6, transcendentals=0),
        compiler_params=pltpu.CompilerParams(vmem_limit_bytes=VMEM),
    )(*operands)


def far_kernel(done, arrays, *refs):
    got = refs[len(done):len(done) + 4 * len(arrays)]
    outs, (slots, sem) = dict(zip(done, refs[len(done) + 4 * len(arrays):])), refs[-2:]
    pieces = []
    for i, a in enumerate(arrays):
        for other in HALVES:
            for h in HALVES:
                src = got[4 * i + 2 * other + h]
                for c, row, b, lo, num in passed_on(h):
                    if c == a and BLOCKS[b][0] in done:
                        pieces.append((src.at[pl.ds(row, num)], rows(outs[BLOCKS[b][0]], b, device_of(3, other), lo, num)))
    stream(pieces, slots, sem, len(pieces))


def far(done, arrays, whole, got):
    any_ = pl.BlockSpec(memory_space=pl.ANY)
    piece, slots = (HALF_WIDE, 12) if 2 not in done else (HALF_TALL, 8)
    operands = [*(whole[w] for w in done), *got]
    return pl.pallas_call(
        functools.partial(far_kernel, done, arrays),
        out_shape=[jax.ShapeDtypeStruct(whole[w].shape, BF) for w in done],
        in_specs=[any_] * len(operands),
        out_specs=[any_] * len(done),
        scratch_shapes=[pltpu.VMEM((slots, *piece), BF), pltpu.SemaphoreType.DMA((slots,))],
        input_output_aliases={i: i for i in range(len(done))},
        cost_estimate=pl.CostEstimate(flops=10**8, bytes_accessed=10**6, transcendentals=0),
        compiler_params=pltpu.CompilerParams(vmem_limit_bytes=VMEM),
    )(*operands)


def solution(mesh):
    swap = [[(i, i ^ bit) for i in range(N)] for bit in (4, 2, 1)]

    def move(array, pairs):
        return lax.ppermute(array, "dp", pairs)

    def step(*arrays):
        out = communicate(*arrays)
        tmp, q, factor, ahead, first = out[:3], out[3:6], out[6], (out[7:11], out[11:15]), [out[15:17]]
        for s in (1, 2, 3):
            first.append([move(ahead[h][s], swap[1 - h]) for h in HALVES])
        second = [[move(one, swap[2]) for one in stage] for stage in first]
        got = [[*first[s], *second[s]] for s in range(4)]
        passed = [*ahead[0], *ahead[1]]
        whole = [None] * 3
        whole[0], whole[2], *moments = settle((0, 2), tmp, passed, (q, factor, arrays[6:9], arrays[9:12]))
        (whole[1],) = settle((1,), tmp, passed, None)
        for w in (0, 1):
            (whole[w],) = far((w,), (0, 1)[w:], whole, [*got[0], *got[1]][4 * w:])
        (whole[2],) = far((2,), (2,), whole, got[2])
        (whole[2],) = far((2,), (3,), whole, got[3])
        return (*whole, *moments)

    all_of, cut = P(None, None, None), P(None, "dp", None)
    return jax.shard_map(
        step,
        mesh=mesh,
        in_specs=(P(("rep", "dp"), None, None, None),) * 3 + (all_of,) * 3 + (cut,) * 6,
        out_specs=(P("rep", None, None),) * 3 + (P("rep", "dp", None),) * 6,
        check_vma=False,
    )
```

```python
import functools

import jax
import jax.numpy as jnp
from jax import lax
from jax.experimental import pallas as pl
from jax.experimental.pallas import tpu as pltpu
from jax.sharding import PartitionSpec as P


D, FF, LAYERS, N = 1024, 3200, 2, 8
COUNT = 3 * LAYERS * D * FF
BLOCKS = ((0, 0), (0, 1), (1, 0), (1, 1), (2, 0), (2, 1))
NB, DOWN = len(BLOCKS), 4
LAST = 144
FIRST = 16
AHEAD = 4
RING = 2
VMEM = 67043328
BF, FL = jnp.bfloat16, jnp.float32
HALVES = (0, 1)
LANES, PACK = 128, 16
TILE = (8, LANES)
WIDE, TALL, HALF_WIDE, HALF_TALL = (128, 3200), (400, 1024), (64, 3200), (208, 1024)
DEPTH = 8
WINDOW = 2


def rows_of(b):
    return (WIDE if b < DOWN else TALL)[0]


def half(b, h):
    rows = rows_of(b)
    split = rows // 2 if b < DOWN else rows // 2 + (8 if b == 4 else -8)
    return (split, rows - split) if h else (0, split)


def tiles(b, num, body, carry):
    full, width = (WIDE[1], 640) if b < DOWN else (TALL[1], 512)

    def one(i, carry):
        at = pl.ds(pl.multiple_of(i * PACK, PACK), PACK)
        for first in range(0, full, width):
            carry = body(at, pl.ds(first, width), width, carry)
        return carry

    return lax.fori_loop(0, num // PACK, one, carry)


def fold(x):
    return sum(x[:, k:k + LANES] for k in range(0, x.shape[1], LANES))


def f32(x):
    return x.astype(FL)


def passed_on(h):
    n4, n5, (l4, l5) = half(4, h)[1], half(5, h)[1], (half(4, h)[0], half(5, h)[0])
    lo, num = half(0, h)
    table = [(0, 0, 0, lo, FIRST), (1, 0, 0, lo + FIRST, num - FIRST)]
    table += [(1, num * b - FIRST, b, half(b, h)[0], num) for b in (1, 2, 3)]
    return table + [(2, 0, 4, l4, n4), (2, n4, 5, l5, n5 - LAST), (3, 0, 5, l5 + n5 - LAST, LAST)]


def kernel(gg, gu, gd, wg, wu, wd, mg, mu, md, vg, vu, vd,
           og, ou, od, qg, qu, qd, fac_out, *rest):
    pass_x, pass_y, land_x, land_y, \
        own_a, own_b, part_a, part_b, rec_a, rec_b, mv_a, mv_b, ws_a, ws_b, sq, nrm, \
        fac, load_sem, d2d_send, d2d_recv, link_send, link_recv, nrm_send, nrm_recv, \
        wmv_sem, out_sem, g_sem, fac_sem = (rest[0:4], rest[4:8], *rest[8:])
    grads, weights, ms, vs, outs, qs = (gg, gu, gd), (wg, wu, wd), (mg, mu, md), (vg, vu, vd), (og, ou, od), (qg, qu, qd)
    me = lax.axis_index("dp")
    x, y, c = lax.div(me, 4), lax.rem(lax.div(me, 2), 2), lax.rem(me, 2)

    def device(r, other=0):
        cx, cy = lax.rem(x + r // 2, 2), lax.rem(y + r % 2, 2)
        return cx * 4 + cy * 2 + (1 - c if other else c)

    def to(index):
        return dict(device_id={"dp": index}, device_id_type=pl.DeviceIdType.MESH)

    across = (device(2), device(1))
    partner = device(0, 1)

    def own(p, r):
        b, _, lo, num = p
        return own_a.at[b, r, pl.ds(lo, num)] if b < DOWN else own_b.at[b - DOWN, r, pl.ds(lo, num)]

    def part(p, r):
        b, _, lo, num = p
        return part_a.at[b, r, pl.ds(lo, num)] if b < DOWN else part_b.at[b - DOWN, r, pl.ds(lo, num)]

    def rec(p, k):
        b, h, lo, num = p
        at = pl.ds(lo - half(b, h)[0], num)
        return rec_a.at[b, h, k, at] if b < DOWN else rec_b.at[b - DOWN, h, k, at]

    def span(ref, p, dev, lead=()):
        b, _, lo, num = p
        w, layer = BLOCKS[b]
        return ref[w].at[(*lead, layer, pl.ds(pl.multiple_of(dev * rows_of(b) + lo, PACK), num))]

    def mine(ref, p):
        b, _, lo, num = p
        return ref[BLOCKS[b][0]].at[BLOCKS[b][1], pl.ds(lo, num)]

    def cut(b, h, *firsts):
        lo, num = half(b, h)
        found = []
        for n in (*firsts, num - sum(firsts)):
            found.append((b, h, lo, n))
            lo += n
        return found

    barrier = pltpu.get_barrier_semaphore()
    for k in range(1, N):
        pl.semaphore_signal(barrier, inc=1, **to(lax.rem(me + k, N)))

    def chip(kind, h):
        return {"S1": 3, "S2": (2, 1)[h], "R": (1, 2)[h], "G": 0}[kind]

    pieces = {}
    for h in HALVES:
        pieces["S1", h] = [p for b in range(NB) for p in (cut(b, h, 16) if b == 0 else cut(b, h))]
        pieces["S2", h] = [p for b in range(NB) for p in cut(b, h)]
        pieces["R", h] = pieces["G", h] = [p for b in range(NB) for p in (cut(b, h, half(b, h)[1] - 48) if b == 5 else cut(b, h))]
    pairs = {kind: list(zip(pieces[kind, 0], pieces[kind, 1], strict=True)) for kind in ("S1", "S2", "R", "G")}
    turns = [("S1", pair) for pair in pairs["S1"]] + [("S2", pair) for pair in pairs["S2"]]
    for n in range(len(pairs["R"]) + 2):
        turns += [("R", pair) for pair in pairs["R"][n:n + 1]] + [("G", pair) for pair in pairs["G"][n - 2:n - 1] if n >= 2]
    units = [(p[0], chip("S1", 0), *p[2:]) for pair in pairs["S1"][:2] for p in pair]
    units += [(b, chip("S1", 0), 0, rows_of(b)) for b in range(1, NB)]
    units += [(b, chip("S2", h), 0, rows_of(b)) for b in range(NB) for h in HALVES]
    units += [(b, 0, 0, rows_of(b)) for b in range(NB)]
    loads, d2ds, here = {}, {}, set()

    def fetch_own(i):
        b, r, lo, num = units[i]
        p = (b, None, lo, num)
        loads[i] = pltpu.make_async_copy(span(grads, p, device(r), (0,)), own(p, r), load_sem.at[i % AHEAD])
        loads[i].start()

    def fetch_part(i):
        b, r, lo, num = units[i]
        p = (b, None, lo, num)
        d2ds[i] = pltpu.make_async_remote_copy(
            span(grads, p, device(r, 1), (0,)), part(p, r), d2d_send.at[i % AHEAD], d2d_recv.at[i], **to(partner))
        d2ds[i].start()

    for i in range(AHEAD):
        fetch_own(i)
    pl.semaphore_wait(barrier, N - 1)
    for i in range(AHEAD):
        fetch_part(i)

    def ready(p, r):
        for i, (b, chip_, lo, num) in enumerate(units):
            if (b, chip_) == (p[0], r) and lo <= p[2] and p[2] + p[3] <= lo + num and i not in here:
                here.add(i)
                loads[i].wait()
                d2ds[i].wait()
                if i + AHEAD < len(units):
                    fetch_own(i + AHEAD)
                    fetch_part(i + AHEAD)

    def add(p, r, terms, squares=False):
        b, _, _, num = p
        target = own(p, r)

        def body(at, cols, width, carry):
            total = f32(target[at, cols])
            for t in terms:
                total = total + f32(t[at, cols])
            rounded = total.astype(BF)
            target[at, cols] = rounded
            return carry + f32(rounded) * f32(rounded) if squares else carry

        width = 640 if b < DOWN else 512
        done = tiles(b, num, body, jnp.zeros((PACK, width), FL) if squares else 0)
        if squares:
            sq[...] += fold(done)

    links, arrivals = [[], []], [{}, {}]

    def send(d, p, r, k):
        i = len(links[d])
        if i >= WINDOW:
            links[d][i - WINDOW].wait_send()
        one = pltpu.make_async_remote_copy(own(p, r), rec(p, k), link_send.at[d, i % WINDOW], link_recv.at[d, i], **to(across[d]))
        one.start()
        links[d].append(one)
        arrivals[d][p, k] = one

    sq[...] = jnp.zeros_like(sq)
    for kind, pair in turns:
        if kind in ("S1", "S2"):
            for h, p in enumerate(pair):
                r = chip(kind, h)
                ready(p, r)
                add(p, r, [part(p, r)])
                send(h, p, r, int(kind == "S2"))

    def slot(b, h, lo=0, num=None):
        at = pl.ds(lo, half(b, h)[1] if num is None else num)
        if b < DOWN:
            return mv_a.at[h, 0, at], mv_a.at[h, 1, at], ws_a.at[h, at]
        return mv_b.at[h, 0, at], mv_b.at[h, 1, at], ws_b.at[h, at]

    states = {}

    def fetch_state(b, h):
        m, v, w = slot(b, h)
        p = cut(b, h)[0]
        states[b, h] = [
            pltpu.make_async_copy(mine(ms, p), m, wmv_sem.at[b // 4, h, 0]),
            pltpu.make_async_copy(mine(vs, p), v, wmv_sem.at[b // 4, h, 1]),
            pltpu.make_async_copy(span(weights, p, me), w, wmv_sem.at[b // 4, h, 2]),
        ]
        for one in states[b, h]:
            one.start()

    for b in (0, 4):
        for h in HALVES:
            fetch_state(b, h)

    keep, waited = {}, set()

    def kept(b):
        if b not in waited:
            waited.add(b)
            keep[b].wait()

    def finish(pair):
        for h, p in enumerate(pair):
            ready(p, 0)
            if (cut(p[0], h)[0], 1) not in waited:
                waited.add((cut(p[0], h)[0], 1))
                arrivals[h][cut(p[0], h)[0], 1].wait_recv()
            arrivals[1 - h][p, 2].wait_recv()
            add(p, 0, [part(p, 0), rec(p, 1), rec(p, 2)], squares=True)
        if pair is pairs["G"][-1] or pair[0][0] != pairs["G"][pairs["G"].index(pair) + 1][0][0]:
            b = pair[0][0]
            if b >= RING:
                kept(b - RING)
            p = (b, None, 0, rows_of(b))
            keep[b] = pltpu.make_async_copy(own(p, 0), mine(qs, p), g_sem.at[b % RING])
            keep[b].start()

    for kind, pair in turns:
        if kind == "G":
            finish(pair)
        elif kind == "R":
            for h, p in enumerate(pair):
                r = chip("R", h)
                ready(p, r)
                for q in pieces["S1", h]:
                    if q[0] == p[0] and (q, 0) not in waited:
                        waited.add((q, 0))
                        arrivals[h][q, 0].wait_recv()
                add(p, r, [part(p, r), rec(p, 0)])
                send(1 - h, p, r, 2)

    nrm[me] = sq[0:8] + sq[8:16]
    sums = []
    for k in range(1, N):
        other = lax.rem(me + k, N)
        one = pltpu.make_async_remote_copy(nrm.at[me], nrm.at[me], nrm_send.at[k], nrm_recv.at[me], **to(other))
        one.start()
        sums.append(one)
    for k in range(1, N):
        other = lax.rem(me + k, N)
        pltpu.make_async_remote_copy(nrm.at[other], nrm.at[other], nrm_send.at[k], nrm_recv.at[other], **to(other)).wait_recv()
    total = nrm[0]
    for k in range(1, N):
        total = total + nrm[k]
    total = jnp.full(TILE, jnp.sum(total), FL)
    fac[...] = jnp.minimum(1.0, 0.5 * lax.rsqrt(total / COUNT + 1e-30))
    fac_copy = pltpu.make_async_copy(fac, fac_out, fac_sem.at[0])
    fac_copy.start()

    def adamw(p):
        b, h, lo, num = p
        if (b, h) not in stepped:
            stepped.add((b, h))
            for one in states[b, h]:
                one.wait()
            kept(b)
        m_ref, v_ref, w_ref = slot(b, h, lo - half(b, h)[0], num)
        target = own(p, 0)

        def body(at, cols, width, carry):
            g = f32(target[at, cols]) * jnp.broadcast_to(fac[0:1, 0:1], (PACK, width))
            m = 0.9 * m_ref[at, cols] + 0.1 * g
            v = 0.95 * v_ref[at, cols] + 0.05 * g * g
            w = f32(w_ref[at, cols])
            step = m * lax.rsqrt(v + 1e-8) + 0.1 * w
            target[at, cols] = (w - 0.02 * step).astype(BF)
            return carry

        tiles(b, num, body, 0)

    stepped = set()
    gats, moves, locals_ = [[], []], [], []
    passes, lands = (pass_x, pass_y), (land_x, land_y)

    def gather_send(d, src, dst, note):
        i = len(gats[d])
        (gats[d][i - WINDOW][0] if i >= WINDOW else links[d][i - WINDOW]).wait_send()
        one = pltpu.make_async_remote_copy(src, dst, link_send.at[d, i % WINDOW], link_recv.at[d, i], **to(across[d]))
        one.start()
        gats[d].append((one, note))

    def hand_over(src, p, dev):
        i = len(moves)
        if i >= AHEAD:
            moves[i - AHEAD].wait_send()
        one = pltpu.make_async_remote_copy(src, span(outs, p, dev), d2d_send.at[i % AHEAD], d2d_recv.at[i], **to(partner))
        one.start()
        moves.append(one)

    def arrived(d, i):
        one, note = gats[d][i]
        one.wait_recv()
        if note is not None:
            ref, p = note
            hand_over(ref, p, across[d])

    def settle_own(b):
        p = (b, None, 0, rows_of(b))
        hand_over(own(p, 0), p, me)
        if b >= RING:
            locals_[b - RING].wait()
        one = pltpu.make_async_copy(own(p, 0), span(outs, p, me), out_sem.at[b % RING])
        one.start()
        locals_.append(one)

    tables = [[(a, row, (b, d, lo, num)) for a, row, b, lo, num in passed_on(d)] for d in HALVES]
    count = len(tables[0])
    for n in range(count + 6):
        for d in HALVES:
            if n < count:
                a, row, p = tables[d][n]
                adamw(p)
                b = p[0]
                if b not in [q[2][0] for q in tables[d][n + 1:]] and b not in (3, 5):
                    fetch_state(b + 1, d)
                ref = passes[d][a].at[pl.ds(row, p[3])]
                gather_send(d, own(p, 0), ref, (ref, p))
            else:
                p = cut(n - count, 1 - d)[0]
                gather_send(d, own(p, 0), span(outs, p, me), (span(outs, p, across[d]), p))
        if n < count and b not in [q[2][0] for q in tables[0][n + 1:]]:
            settle_own(b)
        if n >= WINDOW:
            for d in HALVES:
                arrived(d, n - WINDOW)
    for d in HALVES:
        gather_send(d, passes[1 - d][0], lands[1 - d], None)
    for n in range(count + 4, count + 7):
        for d in HALVES:
            arrived(d, n)

    for d in HALVES:
        for one, _ in gats[d][-WINDOW:]:
            one.wait_send()
    for one in sums:
        one.wait_send()
    for one in locals_[-RING:]:
        one.wait()
    for i, one in enumerate(moves):
        one.wait_recv()
        if i >= len(moves) - AHEAD:
            one.wait_send()
    fac_copy.wait()


ONWARD = [(FIRST, FF), (2 * WIDE[0] - FIRST, FF), (TALL[0] - LAST, D), (LAST, D)]


def communicate(*arrays):
    any_, dma = pl.BlockSpec(memory_space=pl.ANY), pltpu.SemaphoreType.DMA
    wide, tall = [(LAYERS, D, FF)] * 2 + [(LAYERS, FF, D)], [(LAYERS, *WIDE)] * 2 + [(LAYERS, *TALL)]
    shapes = [jax.ShapeDtypeStruct(s, BF) for s in wide + tall] + [jax.ShapeDtypeStruct(TILE, FL)]
    shapes += [jax.ShapeDtypeStruct(s, BF) for s in ONWARD + ONWARD + ONWARD[:1] * 2]
    return pl.pallas_call(
        kernel,
        out_shape=shapes,
        in_specs=[any_] * len(arrays),
        out_specs=[any_] * len(shapes),
        scratch_shapes=[
            *(pltpu.VMEM((4, 4, *WIDE), BF), pltpu.VMEM((2, 4, *TALL), BF)) * 2,
            pltpu.VMEM((4, 2, 3, *HALF_WIDE), BF), pltpu.VMEM((2, 2, 3, *HALF_TALL), BF),
            pltpu.VMEM((2, 2, *HALF_WIDE), FL), pltpu.VMEM((2, 2, *HALF_TALL), FL),
            pltpu.VMEM((2, *HALF_WIDE), BF), pltpu.VMEM((2, *HALF_TALL), BF),
            pltpu.VMEM((PACK, LANES), FL), pltpu.VMEM((N, *TILE), FL), pltpu.VMEM(TILE, FL),
            dma((AHEAD,)), dma((AHEAD,)), dma((34,)), dma((2, WINDOW)), dma((2, 20)), dma((N,)), dma((N,)),
            dma((2, 2, 3)), dma((RING,)), dma((RING,)), dma((1,)),
        ],
        compiler_params=pltpu.CompilerParams(collective_id=0, has_side_effects=True, vmem_limit_bytes=VMEM),
    )(*arrays)


def stream(pieces, slots, sem, depth):
    n, count = len(pieces), slots.shape[0]
    loads = [pltpu.make_async_copy(src, slots.at[i % count, pl.ds(0, src.shape[0])], sem.at[i % count]) for i, (src, _) in enumerate(pieces)]
    stores = [pltpu.make_async_copy(slots.at[i % count, pl.ds(0, dst.shape[0])], dst, sem.at[i % count]) for i, (_, dst) in enumerate(pieces)]
    for i in range(n + depth):
        if i < n:
            if i >= count:
                stores[i - count].wait()
            loads[i].start()
        if i >= depth:
            loads[i - depth].wait()
            stores[i - depth].start()
    for one in stores[max(0, n - count):]:
        one.wait()


def device_of(r, other):
    me = lax.axis_index("dp")
    x, y, c = lax.div(me, 4), lax.rem(lax.div(me, 2), 2), lax.rem(me, 2)
    return lax.rem(x + r // 2, 2) * 4 + lax.rem(y + r % 2, 2) * 2 + (1 - c if other else c)


def rows(ref, b, dev, lo, num):
    return ref.at[BLOCKS[b][1], pl.ds(pl.multiple_of(dev * rows_of(b) + lo, PACK), num)]


def settle_kernel(done, moments, *refs):
    refs = list(refs)
    take = lambda n: [refs.pop(0) for _ in range(n)]
    tmps, passed = dict(zip(done, take(len(done)))), (take(4), take(4))
    qs, fac, ms, vs = (take(3), take(1)[0], take(3), take(3)) if moments else (None,) * 4
    outs = dict(zip(done, take(len(done))))
    new_ms, new_vs = (take(3), take(3)) if moments else (None,) * 2
    wide, tall, mv_a, mv_b, g_a, g_b, factor, c_sem, m_sem, f_sem = refs
    if moments:
        get = pltpu.make_async_copy(fac, factor, f_sem.at[0])
        get.start()

    copies, steps = [], []
    for b in range(NB):
        w, _ = BLOCKS[b]
        if moments:
            steps += [(b, h) for h in HALVES]
        if w not in done:
            continue
        for r in (0, 1, 2):
            for other in HALVES:
                dev = device_of(r, other)
                if r == 0 or other:
                    copies.append((b, rows(tmps[w], b, dev, 0, rows_of(b)), rows(outs[w], b, dev, 0, rows_of(b))))
                    continue
                for h in HALVES:
                    if h == r - 1:
                        lo, num = half(b, h)
                        copies.append((b, rows(tmps[w], b, dev, lo, num), rows(outs[w], b, dev, lo, num)))
                    else:
                        copies += [
                            (b, passed[h][a].at[pl.ds(row, num)], rows(outs[w], b, dev, lo, num))
                            for a, row, c, lo, num in passed_on(h) if c == b
                        ]

    loads, stores, work, users = [], [], [], []
    counts = {}

    def place(kind, slots):
        k = counts.get(kind, 0)
        counts[kind] = k + 1
        return k % slots

    def copy_task(b, src, dst):
        kind, ref, base = ("wide", wide, 0) if b < DOWN else ("tall", tall, wide.shape[0])
        k = place(kind, ref.shape[0])
        mid = ref.at[k, pl.ds(0, src.shape[0])]
        loads.append([pltpu.make_async_copy(src, mid, c_sem.at[base + k])])
        stores.append([pltpu.make_async_copy(mid, dst, c_sem.at[base + k])])
        work.append(None)
        users.append((kind, k))

    def moment_task(b, h):
        kind, mv, gs, base = ("a", mv_a, g_a, 0) if b < DOWN else ("b", mv_b, g_b, mv_a.shape[0])
        k = place(kind, mv.shape[0])
        w, layer = BLOCKS[b]
        lo, num = half(b, h)
        m, v, g = mv.at[k, 0, pl.ds(0, num)], mv.at[k, 1, pl.ds(0, num)], gs.at[k, pl.ds(0, num)]

        def at(refs_):
            return refs_[w].at[layer, pl.ds(lo, num)]

        loads.append([pltpu.make_async_copy(at(x), y, m_sem.at[i, base + k]) for i, (x, y) in enumerate(((ms, m), (vs, v), (qs, g)))])
        stores.append([pltpu.make_async_copy(y, at(x), m_sem.at[i, base + k]) for i, (x, y) in enumerate(((new_ms, m), (new_vs, v)))])
        users.append((kind, k))

        def compute():
            def body(at, cols, width, carry):
                one = f32(g[at, cols]) * jnp.broadcast_to(factor[0:1, 0:1], (PACK, width))
                m[at, cols] = 0.9 * m[at, cols] + 0.1 * one
                v[at, cols] = 0.95 * v[at, cols] + 0.05 * one * one
                return carry

            tiles(b, num, body, 0)

        work.append(compute)

    every = len(copies) / max(len(steps), 1)
    n = 0
    for i, one in enumerate(copies):
        copy_task(*one)
        while n < len(steps) and (n + 0.5) * every <= i + 1:
            moment_task(*steps[n])
            n += 1

    last = {}
    if moments:
        get.wait()
    for i in range(len(users) + DEPTH):
        if i < len(users):
            if users[i] in last:
                for one in stores[last[users[i]]]:
                    one.wait()
            last[users[i]] = i
            for one in loads[i]:
                one.start()
        if 0 <= i - DEPTH < len(users):
            for one in loads[i - DEPTH]:
                one.wait()
            if work[i - DEPTH] is not None:
                work[i - DEPTH]()
            for one in stores[i - DEPTH]:
                one.start()
    for i in last.values():
        for one in stores[i]:
            one.wait()


def settle(done, tmp, passed, moments):
    any_, dma = pl.BlockSpec(memory_space=pl.ANY), pltpu.SemaphoreType.DMA
    operands = [*(tmp[w] for w in done), *passed]
    shapes = [tmp[w] for w in done]
    specs = [any_] * len(operands)
    if moments:
        q, factor, m, v = moments
        operands += [*q, factor, *m, *v]
        specs += [any_] * 10
        shapes += [*m, *v]
    flops = 10**10 * len(done) + (10**10 if moments else 0)
    return pl.pallas_call(
        functools.partial(settle_kernel, done, bool(moments)),
        out_shape=[jax.ShapeDtypeStruct(one.shape, one.dtype) for one in shapes],
        in_specs=specs,
        out_specs=[any_] * len(shapes),
        scratch_shapes=[
            pltpu.VMEM((16, *WIDE), BF), pltpu.VMEM((10, *TALL), BF),
            pltpu.VMEM((5, 2, *HALF_WIDE), FL), pltpu.VMEM((5, 2, *HALF_TALL), FL),
            pltpu.VMEM((5, *HALF_WIDE), BF), pltpu.VMEM((5, *HALF_TALL), BF), pltpu.VMEM(TILE, FL),
            dma((26 if moments else 16,)), dma((3, 10) if moments else (1, 1)), dma((1,)),
        ],
        cost_estimate=pl.CostEstimate(flops=flops, bytes_accessed=30 * 10**6, transcendentals=0),
        compiler_params=pltpu.CompilerParams(vmem_limit_bytes=VMEM),
    )(*operands)


def far_kernel(done, arrays, *refs):
    got = refs[len(done):len(done) + 4 * len(arrays)]
    outs, (slots, sem) = dict(zip(done, refs[len(done) + 4 * len(arrays):])), refs[-2:]
    pieces = []
    for i, a in enumerate(arrays):
        for other in HALVES:
            for h in HALVES:
                src = got[4 * i + 2 * other + h]
                for c, row, b, lo, num in passed_on(h):
                    if c == a and BLOCKS[b][0] in done:
                        pieces.append((src.at[pl.ds(row, num)], rows(outs[BLOCKS[b][0]], b, device_of(3, other), lo, num)))
    stream(pieces, slots, sem, len(pieces))


def far(done, arrays, whole, got):
    any_ = pl.BlockSpec(memory_space=pl.ANY)
    piece, slots = (HALF_WIDE, 12) if 2 not in done else (HALF_TALL, 8)
    operands = [*(whole[w] for w in done), *got]
    return pl.pallas_call(
        functools.partial(far_kernel, done, arrays),
        out_shape=[jax.ShapeDtypeStruct(whole[w].shape, BF) for w in done],
        in_specs=[any_] * len(operands),
        out_specs=[any_] * len(done),
        scratch_shapes=[pltpu.VMEM((slots, *piece), BF), pltpu.SemaphoreType.DMA((slots,))],
        input_output_aliases={i: i for i in range(len(done))},
        cost_estimate=pl.CostEstimate(flops=10**8, bytes_accessed=10**6, transcendentals=0),
        compiler_params=pltpu.CompilerParams(vmem_limit_bytes=VMEM),
    )(*operands)


def solution(mesh):
    swap = [[(i, i ^ bit) for i in range(N)] for bit in (4, 2, 1)]

    def move(array, pairs):
        return lax.ppermute(array, "dp", pairs)

    def step(*arrays):
        out = communicate(*arrays)
        tmp, q, factor, ahead, first = out[:3], out[3:6], out[6], (out[7:11], out[11:15]), [out[15:17]]
        for s in (1, 2, 3):
            first.append([move(ahead[h][s], swap[1 - h]) for h in HALVES])
        second = [[move(one, swap[2]) for one in stage] for stage in first]
        got = [[*first[s], *second[s]] for s in range(4)]
        passed = [*ahead[0], *ahead[1]]
        whole = [None] * 3
        whole[0], whole[2], *moments = settle((0, 2), tmp, passed, (q, factor, arrays[6:9], arrays[9:12]))
        (whole[1],) = settle((1,), tmp, passed, None)
        for w in (0, 1):
            (whole[w],) = far((w,), (0, 1)[w:], whole, [*got[0], *got[1]][4 * w:])
        (whole[2],) = far((2,), (2,), whole, got[2])
        (whole[2],) = far((2,), (3,), whole, got[3])
        return (*whole, *moments)

    all_of, cut = P(None, None, None), P(None, "dp", None)
    return jax.shard_map(
        step,
        mesh=mesh,
        in_specs=(P(("rep", "dp"), None, None, None),) * 3 + (all_of,) * 3 + (cut,) * 6,
        out_specs=(P("rep", None, None),) * 3 + (P("rep", "dp", None),) * 6,
        check_vma=False,
    )
```
